128 devices in a mesh: gx: 8 (over x, core), gy: 16 (over z, y).
Axes of the slice: x: 4, y: 4, z: 4, core: 2. Of those that a mesh axis runs over, the one named last changes fastest.
Arguments:
- state: float32 [1024, 1024, 128], P('gx', 'gy'), may hold values from -6 to 6
- diffusion: float32 [1024, 1024, 128], P('gx', 'gy'), may hold values from 0.01 to 0.12
- vert_inverse: float32 [1024, 128, 128], P('gy'), as said below
- profiles: bfloat16 [131072, 128], P(('gx', 'gy')), may hold values from -6 to 6
- counts: int32 [128, 128], P(('gx', 'gy')), may hold values from 0 to 16, as said below
- cell_lon: int32 [131072], P(('gx', 'gy')), may hold values from 0 to 127
- cell_lat: int32 [131072], P(('gx', 'gy')), may hold values from 0 to 63
- weight_slot: int32 [2, 131072], P(None, ('gx', 'gy')), may hold values from 0 to 63
Outputs:
- adjoint: float32 [1024, 1024, 128], P('gx', 'gy')
The draws below stay inside these ranges and needn't reach their ends.
Inputs may be any that keep to these rules, and one draw needn't show every extreme that they name: Each row s sums to 1024; source device s stores its profiles in order of subdomain, counts[s,d] of them for subdomain d, which covers longitude cells (d // 16) * 128 onwards and latitude cells (d % 16) * 64 onwards. Some subdomain receives 16 profiles from every source. `vert_inverse`: one matrix for each latitude row.
All inputs are finite; a program needn't handle non-finite values.
Results may differ from the reference program's by a relative error of at most 0.0015.
Values may be sent and summed in bfloat16 or wider, within the bound.
A program may use at most 128 MiB of HBM per device.

```python
import math
import jax
import jax.numpy as jnp
from jax import lax

L = 128
CX = 128
CY = 64
CAP = 16
STEPS = 4
SLOTS = 64
NX = 1024
NY = 1024
OBS = 131072
N_GX = 8
N_GY = 16
DEVICES = 128


def draw_vert_inverse(key, part):
    shape = (NY, L, L)
    noise = jax.random.normal(key, shape, jnp.float32)
    return 0.9 * jnp.eye(L, dtype=jnp.float32)[None] + 0.4 * noise / jnp.sqrt(jnp.float32(L))


def draw_counts(key, part):
    half = CAP // 2
    key_heavy = jax.random.fold_in(key, 11)
    key_rows = jax.random.fold_in(key, 12)
    heavy = jax.random.randint(key_heavy, (), 0, DEVICES)
    ids = jnp.arange(DEVICES, dtype=jnp.int32)

    def one_row(row_key):
        key_perm = jax.random.fold_in(row_key, 1)
        key_amount = jax.random.fold_in(row_key, 2)
        order = jax.random.permutation(key_perm, DEVICES).astype(jnp.int32)
        where_heavy = jnp.sum(jnp.where(order == heavy, ids, 0))
        first = order[0]
        order = order.at[where_heavy].set(first).at[0].set(heavy)
        amount = jax.random.randint(key_amount, (DEVICES // 2,), 0, half + 1).astype(jnp.int32)
        amount = amount.at[0].set(half)
        paired = jnp.stack([amount, -amount], axis=1).reshape(DEVICES)
        change = jnp.zeros((DEVICES,), jnp.int32).at[order].set(paired)
        return half + change
    row_keys = jax.random.split(key_rows, DEVICES)
    return jax.vmap(one_row)(row_keys).astype(jnp.int32)


def place_ends(result, stream_key, low, high):
    place = [jax.random.randint(jax.random.fold_in(stream_key, axis), (), 0, length) for axis, length in enumerate(result.shape)]
    widest = result.shape.index(max(result.shape))
    neighbour = place[:widest] + [(place[widest] + 1) % result.shape[widest]] + place[widest + 1:]
    return result.at[tuple(place)].set(low).at[tuple(neighbour)].set(high)


def block_scale(stream_key, extent, cuts, least, top_value):
    def one(axis_at, shards_of):
        draws = jax.random.uniform(jax.random.fold_in(jax.random.fold_in(stream_key, 6), axis_at), (shards_of,), jnp.float32, least / len(cuts), top_value / len(cuts))
        return jnp.repeat(jnp.exp(draws), extent[axis_at] // shards_of).reshape((-1,) + (1,) * (len(extent) - axis_at - 1))

    level = one(*cuts[0])
    for cut in cuts[1:]:
        level = level * one(*cut)
    return level


def gaussian(rng, dims, width, limit, pieces=(), kind=jnp.bfloat16):
    values = width * jax.random.normal(rng, dims, jnp.float32)
    if pieces:
        values = values * block_scale(rng, dims, pieces, -0.22, 0.18)
    return jnp.clip(values, -limit, limit).astype(kind)


def setup_inputs(seed: int = 0) -> dict:
    streams_of = jax.random.split(jax.random.key(seed), 9)
    state = gaussian(streams_of[0], (NX, NY, L), 1.0, 6.0, ((0, 8), (1, 16)), jnp.float32)
    diffusion = jnp.clip(jnp.exp(math.log(0.12) - 2.4849066 * jax.random.uniform(streams_of[1], (NX, NY, L), jnp.float32) ** block_scale(streams_of[1], (NX, NY, L), ((0, 8), (1, 16)), -0.2, 0.2)), 0.01, 0.12)
    vert_inverse = draw_vert_inverse(jax.random.fold_in(streams_of[8], 71), 0)
    profiles = gaussian(streams_of[3], (OBS, L), 1.0, 6.0, ((0, 128),))
    counts = draw_counts(jax.random.fold_in(streams_of[8], 71), 0)
    cell_lon = place_ends(jax.random.randint(streams_of[5], (OBS,), 0, CX), jax.random.fold_in(streams_of[5], 1), 0, CX - 1).astype(jnp.int32)
    cell_lat = place_ends(jax.random.randint(streams_of[6], (OBS,), 0, CY), jax.random.fold_in(streams_of[6], 1), 0, CY - 1).astype(jnp.int32)
    weight_slot = place_ends(jax.random.randint(streams_of[7], (2, OBS), 0, SLOTS), jax.random.fold_in(streams_of[7], 1), 0, SLOTS - 1).astype(jnp.int32)
    return {"state": state, "diffusion": diffusion, "vert_inverse": vert_inverse, "profiles": profiles, "counts": counts, "cell_lon": cell_lon, "cell_lat": cell_lat, "weight_slot": weight_slot}


def reference(state, diffusion, vert_inverse, profiles, counts, cell_lon, cell_lat, weight_slot):
    devices = N_GX * N_GY
    obs_dev = profiles.shape[0] // devices
    cumulative = jnp.cumsum(counts, axis=1)
    positions = jnp.arange(obs_dev, dtype=jnp.int32)
    owner = jax.vmap(lambda row: jnp.searchsorted(row, positions, side="right"))(cumulative)
    owner = owner.reshape(-1).astype(jnp.int32)
    lon_glob = (owner // N_GY) * CX + cell_lon
    lat_glob = (owner % N_GY) * CY + cell_lat
    frac_x = weight_slot[0].astype(jnp.float32) / SLOTS
    frac_y = weight_slot[1].astype(jnp.float32) / SLOTS
    lon_next = (lon_glob + 1) % NX
    lat_next = lat_glob + 1
    inside = (lat_next < NY).astype(jnp.float32)
    lat_next = jnp.minimum(lat_next, NY - 1)
    targets = jnp.concatenate([lon_glob * NY + lat_glob, lon_next * NY + lat_glob,
                               lon_glob * NY + lat_next, lon_next * NY + lat_next])
    weights = jnp.concatenate([(1.0 - frac_x) * (1.0 - frac_y), frac_x * (1.0 - frac_y),
                               (1.0 - frac_x) * frac_y * inside, frac_x * frac_y * inside])
    values = profiles.astype(jnp.float32)
    terms = weights[:, None] * jnp.concatenate([values, values, values, values])
    forcing = jax.ops.segment_sum(terms, targets, num_segments=NX * NY).reshape(NX, NY, -1)
    lam = state + forcing
    for section in range(STEPS):
        mixed = jnp.einsum("xym,ymk->xyk", lam, vert_inverse, precision=lax.Precision.HIGHEST)
        flux = diffusion * mixed
        padded = jnp.pad(flux, ((0, 0), (1, 1), (0, 0)))
        nearby = jnp.roll(flux, 1, axis=0) + jnp.roll(flux, -1, axis=0) + padded[:, 2:] + padded[:, :-2]
        lam = mixed + nearby - 4.0 * flux
    return lam
```

```python
import functools

import jax
import jax.numpy as jnp
from jax import lax
from jax.experimental import pallas as pl
from jax.experimental.pallas import tpu as pltpu
from jax.sharding import PartitionSpec as P

CAP = 16
MESH = pl.DeviceIdType.MESH

ACCS = 4
EDGE = 8
CLEAR = 64


def split(value):
    high = value.astype(jnp.bfloat16)
    low = (value - high.astype(jnp.float32)).astype(jnp.bfloat16)
    return jnp.concatenate([high, low], axis=1)


def exchange_body(n_gx, n_gy, unused_lat, counts_ref, prof_ref, lon_ref, lat_ref, weight_ref, state_ref, diff_ref,
                  inv_ref, prof_out, meta_out, diff_out, inv_out, inv_halo, diff_rows, diff_cols, acc0, acc1, acc2, acc3,
                  counts, prof, lon, lat, weight, wide, table, prof_send, meta_send, inv_stage, state_stage, diff_stage, row_stage, high_stage,
                  load_sem, psend, precv, msend, mrecv, hsend, hrecv):
    held, levels = prof_ref.shape
    peers = prof_out.shape[0]
    nx, ny, _ = state_ref.shape
    pitch = state_stage.shape[0] // nx
    wide_x = nx + EDGE
    gx = lax.axis_index("gx")
    gy = lax.axis_index("gy")
    me = gx * n_gy + gy
    small = [
        pltpu.make_async_copy(src, dst, load_sem.at[k])
        for k, (src, dst) in enumerate(
            [(counts_ref, counts), (prof_ref, prof), (lon_ref, lon), (lat_ref, lat), (weight_ref, weight)])
    ]
    large = [
        pltpu.make_async_copy(diff_ref, diff_stage.reshape(nx, pitch, levels).at[:, 0:ny, :], load_sem.at[5]),
        pltpu.make_async_copy(inv_ref, inv_stage, load_sem.at[6]),
        pltpu.make_async_copy(state_ref, state_stage.reshape(nx, pitch, levels).at[:, 0:ny, :], load_sem.at[7]),
    ]
    for copy in small + large:
        copy.start()

    def peer(i):
        y = lax.rem(lax.rem(gy, 4) + lax.rem(i, 4) + 2, 4)
        z = lax.rem(lax.div(gy, 4) + lax.rem(lax.div(i, 4), 4) + n_gy // 8, n_gy // 4)
        x = lax.rem(lax.div(gx, 2) + lax.rem(lax.div(i, n_gy), n_gx // 2) + n_gx // 4, n_gx // 2)
        c = lax.rem(gx + lax.div(i, n_gy * (n_gx // 2)), 2)
        return x * 2 + c, z * 4 + y

    own = 2 + (n_gy // 8) * 4 + (n_gx // 4) * n_gy

    def each_peer(do):
        for first, last in ((0, own), (own + 1, peers)):

            @pl.loop(first, last)
            def _(i):
                do(*peer(i))

    barrier = pltpu.get_barrier_semaphore()
    each_peer(lambda x, y: pl.semaphore_signal(barrier, inc=1, device_id=(x, y), device_id_type=MESH))

    for copy in small:
        copy.wait()
    blocks = held // 128
    wide[0:held, :] = prof[...].astype(jnp.float32)
    wide[held:held + CAP, :] = jnp.zeros((CAP, levels), jnp.float32)
    for b in range(blocks):
        table[b, 0:1, :] = lon[b:b + 1, :]
        table[b, 1:2, :] = lat[b:b + 1, :]
        table[b, 2:4, :] = weight[:, b * 128:(b + 1) * 128]
        table[b, 4:8, :] = jnp.zeros((4, 128), jnp.int32)
    for b in range(blocks, blocks + 2):
        table[b] = jnp.zeros((8, 128), jnp.int32)
    lane = lax.broadcasted_iota(jnp.int32, (8, 128), 1)
    field = lax.broadcasted_iota(jnp.int32, (8, 128), 0)

    def one(d, start):
        count = counts[0, d]
        prof_send[d] = wide[pl.ds(start, CAP), :].astype(jnp.bfloat16)
        at = lax.rem(start, 128)
        b = lax.div(start, 128)
        back = lax.rem(128 - at, 128)
        here = pltpu.roll(table[b], back, 1)
        there = pltpu.roll(table[b + 1], back, 1)
        got = jnp.where(lane < 128 - at, here, there)
        got = jnp.where((field == 1) & (lane >= count), unused_lat, got)
        row = jnp.where((field == 0) & (lane < CAP), got, 0)
        for f in range(1, 4):
            moved = pltpu.roll(got, f * CAP, 1)
            row = row + jnp.where((field == f) & (lane >= f * CAP) & (lane < (f + 1) * CAP), moved, 0)
        meta_send[pl.ds(d, 1), :] = jnp.sum(row, axis=0, keepdims=True)
        return start + count

    lax.fori_loop(0, peers, one, jnp.int32(0), unroll=16)

    def remote(src, dst, ssem, rsem, x, y):
        return pltpu.make_async_remote_copy(
            src_ref=src, dst_ref=dst, send_sem=ssem, recv_sem=rsem, device_id=(x, y), device_id_type=MESH)

    has_n = gy < n_gy - 1
    has_s = gy > 0
    up = jnp.minimum(gy + 1, n_gy - 1)
    down = jnp.maximum(gy - 1, 0)
    e = lax.rem(gx + 1, n_gx)
    w = lax.rem(gx + n_gx - 1, n_gx)

    def halo(k, src, dst, x, y):
        return remote(src, dst, hsend.at[k], hrecv.at[k], x, y)

    to_e = halo(0, diff_stage.at[(nx - 1) * pitch:(nx - 1) * pitch + ny], diff_cols.at[0], e, gy)
    to_w = halo(1, diff_stage.at[0:ny], diff_cols.at[1], w, gy)
    to_n = [halo(2, row_stage.at[1], diff_rows.at[1], gx, up),
            halo(3, high_stage.at[1], inv_halo.at[1], gx, up)]
    to_s = [halo(4, row_stage.at[0], diff_rows.at[0], gx, down),
            halo(5, high_stage.at[0], inv_halo.at[0], gx, down)]
    large[0].wait()
    large[1].wait()
    for k, y in ((0, 0), (1, ny - 1)):
        row_stage[k] = diff_stage[pl.ds(y, nx, stride=pitch), :].astype(jnp.bfloat16)
        high_stage[k] = inv_stage[y].astype(jnp.bfloat16)
    pl.semaphore_wait(barrier, peers - 1)

    def send(x, y):
        to = x * n_gy + y
        remote(prof_send.at[to], prof_out.at[me], psend, precv, x, y).start()
        remote(meta_send.at[pl.ds(to, 1)], meta_out.at[pl.ds(me, 1)], msend, mrecv, x, y).start()

    each_peer(send)
    to_e.start()
    to_w.start()

    @pl.when(has_n)
    def _():
        for copy in to_n:
            copy.start()

    @pl.when(has_s)
    def _():
        for copy in to_s:
            copy.start()

    prof_out[me] = prof_send[me]
    meta_out[pl.ds(me, 1), :] = meta_send[pl.ds(me, 1), :]
    empty = jnp.zeros((CLEAR, levels), jnp.float32)

    @pl.loop(0, acc1.shape[0] // CLEAR)
    def _(i):
        rows = pl.ds(pl.multiple_of(i * CLEAR, CLEAR), CLEAR)
        for acc in (acc1, acc2, acc3):
            acc[rows, :] = empty

    @pl.loop(0, ny, unroll=4)
    def _(y):
        inv_out[y] = split(inv_stage[y])

    large[2].wait()
    margin = jnp.zeros((EDGE, levels), jnp.float32)

    @pl.loop(0, ny, unroll=2)
    def _(y):
        first = pl.multiple_of(y * wide_x, 8)
        acc0[pl.ds(first, nx), :] = state_stage[pl.ds(y, nx, stride=pitch), :]
        acc0[pl.ds(first + nx, EDGE), :] = margin
        diff_out[y] = diff_stage[pl.ds(y, nx, stride=pitch), :]

    tail = acc0.shape[0] - ny * wide_x
    acc0[ny * wide_x:, :] = jnp.zeros((tail, levels), jnp.float32)
    n = peers - 1
    whole_p = remote(prof_send.at[0:n], prof_out.at[0:n], psend, precv, gx, gy)
    whole_m = remote(meta_send.at[0:n], meta_out.at[0:n], msend, mrecv, gx, gy)
    whole_p.wait_recv()
    whole_m.wait_recv()
    whole_p.wait_send()
    whole_m.wait_send()
    for copy in (to_e, to_w):
        copy.wait_send()
        copy.wait_recv()

    @pl.when(has_n)
    def _():
        for copy in to_n:
            copy.wait_send()
        for copy in to_s:
            copy.wait_recv()

    @pl.when(has_s)
    def _():
        for copy in to_s:
            copy.wait_send()
        for copy in to_n:
            copy.wait_recv()


def exchange(counts, prof, lon, lat, weight, state, diff, inv, unused_lat, n_gx, n_gy):
    held, levels = prof.shape
    nx, ny, _ = state.shape
    peers = counts.shape[1]
    vm = pltpu.VMEM
    dma = pltpu.SemaphoreType.DMA
    hbm = functools.partial(pltpu.with_memory_space_constraint, memory_space=pltpu.HBM)
    args = (counts, prof, lon.reshape(-1, 128), lat.reshape(-1, 128), weight, state, diff, inv)
    pitched = (nx * (ny + 8), levels)
    rows = -(-(ny + 3) * (nx + EDGE) // CLEAR) * CLEAR
    return pl.pallas_call(
        functools.partial(exchange_body, n_gx, n_gy, unused_lat),
        out_shape=(
            vm((peers, CAP, levels), jnp.bfloat16),
            vm((peers, 128), jnp.int32),
            vm((ny, nx, levels), jnp.float32),
            vm((ny, levels, 2 * levels), jnp.bfloat16),
            vm((2, levels, levels), jnp.bfloat16),
            vm((2, nx, levels), jnp.bfloat16),
            vm((2, ny, levels), jnp.float32),
            *[vm((rows, levels), jnp.float32)] * ACCS,
        ),
        in_specs=[pl.BlockSpec(memory_space=pltpu.HBM)] * 8,
        out_specs=[pl.BlockSpec(memory_space=vm)] * (7 + ACCS),
        scratch_shapes=[
            pltpu.SMEM((1, peers), jnp.int32),
            vm((held, levels), jnp.bfloat16),
            vm((held // 128, 128), jnp.int32),
            vm((held // 128, 128), jnp.int32),
            vm((2, held), jnp.int32),
            vm((held + CAP, levels), jnp.float32),
            vm((held // 128 + 2, 8, 128), jnp.int32),
            vm((peers, CAP, levels), jnp.bfloat16),
            vm((peers, 128), jnp.int32),
            vm((ny, levels, levels), jnp.float32),
            vm(pitched, jnp.float32),
            vm(pitched, jnp.float32),
            vm((2, nx, levels), jnp.bfloat16),
            vm((2, levels, levels), jnp.bfloat16),
            dma((8,)), dma, dma, dma, dma, dma((6,)), dma((6,)),
        ],
        compiler_params=pltpu.CompilerParams(
            collective_id=0, has_side_effects=True, vmem_limit_bytes=17 * 1024 * 1024),
        name="exchange",
    )(*[hbm(a) for a in args])


SLOTS = 64


def scatter_body(nx, ny, prof_ref, meta_ref, *rest):
    peers, cap, levels = prof_ref.shape
    pitch = nx + EDGE
    accs = rest[ACCS:2 * ACCS]
    edge_e, edge_w, edge_n, edge_s, knot, table, index_v, index_s, index_sem = rest[2 * ACCS:]
    meta = meta_ref[...]
    lat_up = pltpu.roll(meta, 128 - cap, 1)
    index_v[...] = lat_up * pitch + meta
    index_copy = pltpu.make_async_copy(index_v, index_s, index_sem)
    index_copy.start()
    group = 8
    lane = lax.broadcasted_iota(jnp.int32, (group, cap, 128), 2)
    slot = lax.broadcasted_iota(jnp.int32, (group, cap, 128), 1)
    own = (lane % cap == slot).astype(jnp.float32)
    r = lax.broadcasted_iota(jnp.int32, (128, 2 * levels), 0) // cap
    c = lax.broadcasted_iota(jnp.int32, (128, 2 * levels), 1) // levels
    pick = (r == c + 2).astype(jnp.bfloat16)

    @pl.loop(0, peers // group, unroll=4)
    def _(i):
        m = meta_ref[pl.ds(pl.multiple_of(i * group, group), group), :].astype(jnp.float32)
        spread = (m[:, None, :] * own).reshape(group * cap, 128).astype(jnp.bfloat16)
        frac = jnp.dot(spread, pick, preferred_element_type=jnp.float32) * (1.0 / SLOTS)
        fx = frac[:, :levels]
        fy = frac[:, levels:]
        p = prof_ref[pl.ds(i * group, group)].reshape(group * cap, levels).astype(jnp.float32)
        p1 = p * fx
        p0 = p - p1
        q01 = p0 * fy
        q11 = p1 * fy
        base = i * (group * cap * 4)
        n = group * cap
        table[pl.ds(base, n, stride=4), :] = p0 - q01
        table[pl.ds(base + 1, n, stride=4), :] = p1 - q11
        table[pl.ds(base + 2, n, stride=4), :] = q01
        table[pl.ds(base + 3, n, stride=4), :] = q11

    index_copy.wait()

    @pl.loop(0, peers)
    def _(s):
        first = pl.multiple_of(s * (cap * 4), cap * 4)
        for k in range(0, cap, ACCS):
            for j in range(ACCS):
                at = index_s[s, k + j]
                row = first + (k + j) * 4
                acc = accs[j]
                acc[pl.ds(at, 2), :] += table[pl.ds(row, 2), :]
                acc[pl.ds(at + pitch, 2), :] += table[pl.ds(row + 2, 2), :]

    def total(at, n):
        out = accs[0][pl.ds(at, n), :]
        for acc in accs[1:]:
            out = out + acc[pl.ds(at, n), :]
        return out

    @pl.loop(0, ny, unroll=8)
    def _(y):
        first = pl.multiple_of(y * pitch, 8)
        edge_w[pl.ds(y, 1), :] = total(first, 8)[0:1]
        edge_e[pl.ds(y, 1), :] = total(first + nx - 8, 8)[7:8]
        edge_e[pl.ds(ny + y, 1), :] = total(first + nx, 8)[0:1]

    edge_s[...] = total(0, nx).astype(edge_s.dtype)
    edge_n[0] = total((ny - 1) * pitch, nx).astype(edge_n.dtype)
    edge_n[1] = total(ny * pitch, nx).astype(edge_n.dtype)
    corner = total(ny * pitch + nx, 8)
    edge_e[2 * ny:2 * ny + 8, :] = corner
    knot[0:1, :] = corner[0:1]
    knot[1:2, :] = total((ny - 1) * pitch + nx, 8)[0:1]
    knot[2:3, :] = total(ny * pitch + nx - 8, 8)[7:8]
    knot[3:4, :] = total(nx, 8)[0:1]
    knot[4:5, :] = total(ny * pitch, 8)[0:1]
    knot[5:8, :] = jnp.zeros((3, levels), jnp.float32)


def scatter(prof, meta, accs, nx, ny):
    peers, cap, levels = prof.shape
    vm = pltpu.VMEM
    block = pl.BlockSpec(memory_space=vm)
    return pl.pallas_call(
        functools.partial(scatter_body, nx, ny),
        out_shape=(
            *[vm(accs[0].shape, jnp.float32)] * ACCS,
            vm((2 * ny + 8, levels), jnp.float32),
            vm((ny, levels), jnp.float32),
            vm((2, nx, levels), jnp.bfloat16),
            vm((nx, levels), jnp.bfloat16),
            vm((8, levels), jnp.float32),
        ),
        in_specs=[block] * (2 + ACCS),
        out_specs=[block] * (5 + ACCS),
        scratch_shapes=[
            vm((peers * cap * 4 + 8, levels), jnp.float32),
            vm((peers, 128), jnp.int32),
            pltpu.SMEM((peers, 128), jnp.int32),
            pltpu.SemaphoreType.DMA,
        ],
        input_output_aliases={2 + k: k for k in range(ACCS)},
        compiler_params=pltpu.CompilerParams(vmem_limit_bytes=5 * 1024 * 1024),
        name="scatter",
    )(prof, meta, *accs)


STEPS = 4
CHUNK = 16


def steps_body(n_gx, n_gy, acc0, acc1, acc2, acc3, edge_e, edge_w, edge_n, edge_s, knot,
               diff_ref, inv_pair, inv_halo, diff_rows, diff_cols, out_ref,
               mu_ref, g_last, g_other, col_send, col_recv, row_send, row_recv, in_w, in_e, in_s, in_n, knots,
               spill_send, spill_recv, col_ssem, col_rsem, row_ssem, row_rsem):
    ny, nx, levels = diff_ref.shape
    pitch = nx + EDGE
    gx = lax.axis_index("gx")
    gy = lax.axis_index("gy")
    e = lax.rem(gx + 1, n_gx)
    w = lax.rem(gx + n_gx - 1, n_gx)
    has_n = gy < n_gy - 1
    has_s = gy > 0
    up = jnp.minimum(gy + 1, n_gy - 1)
    down = jnp.maximum(gy - 1, 0)
    barrier = pltpu.get_barrier_semaphore()

    def greet(x, y):
        pl.semaphore_signal(barrier, inc=1, device_id=(x, y), device_id_type=MESH)

    greet(e, gy)
    greet(w, gy)

    @pl.when(has_n)
    def _():
        greet(gx, up)
        greet(e, up)
        greet(w, up)

    @pl.when(has_s)
    def _():
        greet(gx, down)
        greet(e, down)
        greet(w, down)

    pl.semaphore_wait(barrier, 2 + 3 * has_n.astype(jnp.int32) + 3 * has_s.astype(jnp.int32))

    def remote(src, dst, ssem, rsem, x, y):
        return pltpu.make_async_remote_copy(
            src_ref=src, dst_ref=dst, send_sem=ssem, recv_sem=rsem, device_id=(x, y), device_id_type=MESH)

    def spill(k, src, dst, x, y):
        return remote(src, dst, spill_send.at[k], spill_recv.at[k], x, y)

    across = [spill(0, edge_e, in_w, e, gy), spill(1, edge_w, in_e, w, gy)]
    north_to = [spill(2, edge_n, in_s, gx, up), spill(4, knot, knots.at[0], e, up),
                spill(6, knot, knots.at[2], w, up), spill(7, knot, knots.at[3], gx, up)]
    south_to = [spill(3, edge_s, in_n, gx, down), spill(5, knot, knots.at[1], e, down)]
    for copy in across:
        copy.start()

    @pl.when(has_n)
    def _():
        for copy in north_to:
            copy.start()

    @pl.when(has_s)
    def _():
        for copy in south_to:
            copy.start()

    zeros = jnp.zeros((nx + 2 * EDGE, levels), jnp.float32)

    @pl.when(jnp.logical_not(has_s))
    def _():
        g_other[0] = zeros
        g_last[0] = zeros

    @pl.when(jnp.logical_not(has_n))
    def _():
        g_other[ny + 1] = zeros
        g_last[ny + 1] = zeros

    chunks = ny // CHUNK

    def cols(n, side, c):
        rows = pl.ds(pl.multiple_of(c * CHUNK, CHUNK), CHUNK)
        return remote(col_send.at[n, side, rows], col_recv.at[n, side, rows],
                      col_ssem.at[n, side, c], col_rsem.at[n, side, c], e if side == 0 else w, gy)

    def flux(n):
        return g_last if (STEPS - 1 - n) % 2 == 0 else g_other

    def rowcopy(n, side):
        return remote(row_send.at[n, side], row_recv.at[n, side],
                      row_ssem.at[n, side], row_rsem.at[n, side], gx, up if side == 0 else down)

    def stencil(g, y):
        mid = g[y + 1, pl.ds(EDGE, nx), :]
        near = (g[y + 1, pl.ds(EDGE - 1, nx), :] + g[y + 1, pl.ds(EDGE + 1, nx), :]) + (
            g[y, pl.ds(EDGE, nx), :] + g[y + 2, pl.ds(EDGE, nx), :])
        return mu_ref[y] + (near - 4.0 * mid)

    first_lane = lax.broadcasted_iota(jnp.int32, (8, levels), 0) == 0

    side_lane = lax.broadcasted_iota(jnp.int32, (16, levels), 0)

    def sides(y):
        spilled = in_w[pl.ds(ny + y, 1), :]
        west = in_w[pl.ds(y, 1), :]
        east = in_e[pl.ds(y, 1), :] + edge_e[pl.ds(ny + y, 1), :]
        lam = jnp.where(side_lane == 0, spilled, jnp.where(side_lane == 1, west, jnp.where(side_lane == 2, east, 0.0)))
        mu = jnp.dot(lam.astype(jnp.bfloat16), inv_pair[y, :, 0:levels], preferred_element_type=jnp.float32)
        g = flux(0)
        mu_ref[y, 0:1, :] += mu[0:1]
        g[y + 1, EDGE:EDGE + 1, :] += diff_ref[y, 0:1, :] * mu[0:1]
        g[y + 1, EDGE - 1:EDGE, :] = diff_cols[0, pl.ds(y, 1), :] * mu[1:2]
        g[y + 1, EDGE + nx:EDGE + nx + 1, :] = diff_cols[1, pl.ds(y, 1), :] * mu[2:3]

    def beside(lam, extra):
        head = lam[0:8] + jnp.where(first_lane, extra, 0.0)
        return jnp.concatenate([head, lam[8:]], axis=0).astype(jnp.bfloat16)

    def mixed(lam, y):
        pair = inv_pair[y]
        both = jnp.dot(split(lam), jnp.concatenate([pair, pair], axis=0), preferred_element_type=jnp.float32)
        mu = both[:, :levels] + both[:, levels:]
        return mu, diff_ref[y] * mu

    def neighbours_in():
        @pl.when(has_s)
        def _():
            for copy in north_to:
                copy.wait_recv()
            fresh, g = mixed(in_s[1].astype(jnp.float32), 0)
            mu_ref[0] += fresh
            flux(0)[1, EDGE:EDGE + nx, :] += g
            in_w[ny:ny + 1, :] += knots[0, 0:1, :]
            in_w[0:1, :] += knots[0, 2:3, :]
            in_e[0:1, :] += knots[2, 4:5, :] + knots[3, 0:1, :]
            lam = beside(in_s[0].astype(jnp.float32), knots[0, 1:2, :])
            mu = jnp.dot(lam, inv_halo[1], preferred_element_type=jnp.float32)
            flux(0)[0, EDGE:EDGE + nx, :] = diff_rows[1].astype(jnp.float32) * mu

        @pl.when(has_n)
        def _():
            for copy in south_to:
                copy.wait_recv()
            lam = beside(in_n[...].astype(jnp.float32) + edge_n[1].astype(jnp.float32),
                         knots[1, 3:4, :] + in_w[2 * ny:2 * ny + 1, :])
            mu = jnp.dot(lam, inv_halo[0], preferred_element_type=jnp.float32)
            flux(0)[ny + 1, EDGE:EDGE + nx, :] = diff_rows[0].astype(jnp.float32) * mu

    def row(n, y):
        if n > 0:
            return mixed(stencil(flux(n - 1), y), y)
        rows = pl.ds(pl.multiple_of(y * pitch, 8), nx)
        return mixed((acc0[rows, :] + acc1[rows, :]) + (acc2[rows, :] + acc3[rows, :]), y)

    def columns_in(n, c):
        for side in range(2):
            cols(n, side, c).wait_recv()
        for r in range(CHUNK):
            y = c * CHUNK + r
            flux(n)[y + 1, EDGE - 1:EDGE, :] = col_recv[n, 0, pl.ds(y, 1), :]
            flux(n)[y + 1, EDGE + nx:EDGE + nx + 1, :] = col_recv[n, 1, pl.ds(y, 1), :]

    def rows_in(n):
        @pl.when(has_s)
        def _():
            rowcopy(n, 0).wait_recv()
            flux(n)[0, EDGE:EDGE + nx, :] = row_recv[n, 0].astype(jnp.float32)

        @pl.when(has_n)
        def _():
            rowcopy(n, 1).wait_recv()
            flux(n)[ny + 1, EDGE:EDGE + nx, :] = row_recv[n, 1].astype(jnp.float32)

    def north_out(n):
        @pl.when(has_n)
        def _():
            rowcopy(n, 0).start()

    def south_out(n):
        @pl.when(has_s)
        def _():
            rowcopy(n, 1).start()

    for n in range(STEPS):
        if n > 0:
            if n > 1:
                columns_in(n - 1, chunks - 1)
                columns_in(n - 1, 0)
                rows_in(n - 1)
            row_send[n, 0] = row(n, ny - 1)[1].astype(row_send.dtype)
            row_send[n, 1] = row(n, 0)[1].astype(row_send.dtype)
            north_out(n)
            south_out(n)

        @pl.loop(0, chunks)
        def _(i):
            c = lax.rem(i + chunks - 1, chunks)
            if n > 1:

                @pl.when(i > 1)
                def _():
                    columns_in(n - 1, c)

            for r in range(CHUNK):
                y = c * CHUNK + r
                mu, g = row(n, y)
                mu_ref[y] = mu
                flux(n)[y + 1, pl.ds(EDGE, nx), :] = g
                if n > 0:
                    col_send[n, 0, pl.ds(y, 1), :] = g[nx - 1:nx]
                    col_send[n, 1, pl.ds(y, 1), :] = g[0:1]

            if n > 0:
                for side in range(2):
                    cols(n, side, c).start()

        if n == 0:
            for copy in across:
                copy.wait_recv()

            @pl.loop(0, chunks)
            def _(i):
                c = chunks - 1 - i
                pl.when(i == chunks - 1)(neighbours_in)
                for r in range(CHUNK):
                    sides(c * CHUNK + r)

    last = STEPS - 1

    out_pitch = out_ref.shape[0] // nx
    nothing = jnp.zeros((1, levels), jnp.float32)
    g_last[0] = zeros
    g_last[ny + 1] = zeros

    @pl.loop(0, chunks)
    def _(c):
        for r in range(CHUNK):
            y = c * CHUNK + r
            g_last[y + 1, EDGE - 1:EDGE, :] = nothing
            g_last[y + 1, EDGE + nx:EDGE + nx + 1, :] = nothing

    @pl.loop(0, chunks)
    def _(c):
        for r in range(CHUNK):
            y = c * CHUNK + r
            out_ref[pl.ds(y, nx, stride=out_pitch), :] = stencil(g_last, y)

    @pl.loop(0, chunks)
    def _(c):
        for side in range(2):
            cols(last, side, c).wait_recv()

    east_edge = (nx - 1) * out_pitch
    out_ref[0:ny, :] += col_recv[last, 0]
    out_ref[east_edge:east_edge + ny, :] += col_recv[last, 1]

    @pl.when(has_s)
    def _():
        rowcopy(last, 0).wait_recv()
        out_ref[pl.ds(0, nx, stride=out_pitch), :] += row_recv[last, 0].astype(jnp.float32)

    @pl.when(has_n)
    def _():
        rowcopy(last, 1).wait_recv()
        out_ref[pl.ds(ny - 1, nx, stride=out_pitch), :] += row_recv[last, 1].astype(jnp.float32)

    @pl.when(has_s)
    def _():
        for n in range(1, STEPS):
            rowcopy(n, 1).wait_send()
        for copy in south_to:
            copy.wait_send()

    @pl.when(has_n)
    def _():
        for n in range(1, STEPS):
            rowcopy(n, 0).wait_send()
        for copy in north_to:
            copy.wait_send()

    for copy in across:
        copy.wait_send()
    for n in range(1, STEPS):

        @pl.loop(0, chunks)
        def _(c):
            for side in range(2):
                cols(n, side, c).wait_send()


def steps(accs, edges, diffusion, inverse, halos, n_gx, n_gy, space=None):
    ny, nx, levels = diffusion.shape
    vm = pltpu.VMEM
    chunks = ny // CHUNK
    dma = pltpu.SemaphoreType.DMA
    make = space or (lambda s, d: jax.ShapeDtypeStruct(s, d))
    return pl.pallas_call(
        functools.partial(steps_body, n_gx, n_gy),
        out_shape=make((nx * (ny + 8), levels), jnp.float32),
        in_specs=[pl.BlockSpec(memory_space=vm)] * (10 + ACCS),
        out_specs=pl.BlockSpec(memory_space=vm),
        scratch_shapes=[
            vm((ny, nx, levels), jnp.float32),
            vm((ny + 2, nx + 2 * EDGE, levels), jnp.float32),
            vm((ny + 2, nx + 2 * EDGE, levels), jnp.float32),
            vm((STEPS, 2, ny, levels), jnp.float32),
            vm((STEPS, 2, ny, levels), jnp.float32),
            vm((STEPS, 2, nx, levels), jnp.bfloat16),
            vm((STEPS, 2, nx, levels), jnp.bfloat16),
            vm((2 * ny + 8, levels), jnp.float32),
            vm((ny, levels), jnp.float32),
            vm((2, nx, levels), jnp.bfloat16),
            vm((nx, levels), jnp.bfloat16),
            vm((4, 8, levels), jnp.float32),
            dma((8,)), dma((8,)),
            dma((STEPS, 2, chunks)), dma((STEPS, 2, chunks)), dma((STEPS, 2)), dma((STEPS, 2)),
        ],
        compiler_params=pltpu.CompilerParams(
            collective_id=1, has_side_effects=True, vmem_limit_bytes=17 * 1024 * 1024),
        name="steps",
    )(*accs, *edges, diffusion, inverse, *halos)


def finish_body(parts, stage, out_ref, sems):
    nx, ny, levels = out_ref.shape
    wide = stage.reshape(nx, stage.shape[0] // nx, levels)
    step = nx // parts
    copies = [
        pltpu.make_async_copy(wide.at[k * step:(k + 1) * step, 0:ny, :], out_ref.at[k * step:(k + 1) * step], sems.at[k])
        for k in range(parts)
    ]
    for copy in copies:
        copy.start()
    for copy in copies:
        copy.wait()


def finish(stage, nx, ny):
    levels = stage.shape[1]
    parts = 8
    return pl.pallas_call(
        functools.partial(finish_body, parts),
        out_shape=jax.ShapeDtypeStruct((nx, ny, levels), jnp.float32),
        in_specs=[pl.BlockSpec(memory_space=pltpu.VMEM)],
        out_specs=pl.BlockSpec(memory_space=pltpu.HBM),
        scratch_shapes=[pltpu.SemaphoreType.DMA((parts,))],
        compiler_params=pltpu.CompilerParams(vmem_limit_bytes=1024 * 1024),
        name="finish",
    )(stage)


def shards(n_gx, n_gy, state, diffusion, vert_inverse, profiles, counts, cell_lon, cell_lat, weight_slot):
    nx, ny, _ = state.shape
    got, got_meta, diffusion, inverse, *rest = exchange(
        counts, profiles, cell_lon, cell_lat, weight_slot, state, diffusion, vert_inverse, ny + 1, n_gx, n_gy)
    made = scatter(got, got_meta, rest[3:], nx, ny)
    stage = steps(made[:ACCS], made[ACCS:], diffusion, inverse, rest[:3], n_gx, n_gy, pltpu.VMEM)
    return finish(stage, nx, ny)


def solution(mesh):
    return jax.shard_map(
        functools.partial(shards, mesh.shape["gx"], mesh.shape["gy"]),
        mesh=mesh,
        in_specs=(
            P("gx", "gy", None),
            P("gx", "gy", None),
            P("gy", None, None),
            P(("gx", "gy"), None),
            P(("gx", "gy"), None),
            P(("gx", "gy")),
            P(("gx", "gy")),
            P(None, ("gx", "gy")),
        ),
        out_specs=P("gx", "gy", None),
        check_vma=False,
    )
```

```python
import functools

import jax
import jax.numpy as jnp
from jax import lax
from jax.experimental import pallas as pl
from jax.experimental.pallas import tpu as pltpu
from jax.sharding import PartitionSpec as P

CAP = 16
MESH = pl.DeviceIdType.MESH

ACCS = 4
EDGE = 8
CLEAR = 64


def split(value):
    high = value.astype(jnp.bfloat16)
    low = (value - high.astype(jnp.float32)).astype(jnp.bfloat16)
    return jnp.concatenate([high, low], axis=1)


def exchange_body(n_gx, n_gy, unused_lat, counts_ref, prof_ref, lon_ref, lat_ref, weight_ref, state_ref, diff_ref,
                  inv_ref, prof_out, meta_out, diff_out, inv_out, inv_halo, diff_rows, diff_cols, acc0, acc1, acc2, acc3,
                  counts, prof, lon, lat, weight, wide, table, prof_send, meta_send, inv_stage, state_stage, diff_stage, row_stage, high_stage,
                  load_sem, psend, precv, msend, mrecv, hsend, hrecv):
    held, levels = prof_ref.shape
    peers = prof_out.shape[0]
    nx, ny, _ = state_ref.shape
    pitch = state_stage.shape[0] // nx
    wide_x = nx + EDGE
    gx = lax.axis_index("gx")
    gy = lax.axis_index("gy")
    me = gx * n_gy + gy
    small = [
        pltpu.make_async_copy(src, dst, load_sem.at[k])
        for k, (src, dst) in enumerate(
            [(counts_ref, counts), (prof_ref, prof), (lon_ref, lon), (lat_ref, lat), (weight_ref, weight)])
    ]
    large = [
        pltpu.make_async_copy(diff_ref, diff_stage.reshape(nx, pitch, levels).at[:, 0:ny, :], load_sem.at[5]),
        pltpu.make_async_copy(inv_ref, inv_stage, load_sem.at[6]),
        pltpu.make_async_copy(state_ref, state_stage.reshape(nx, pitch, levels).at[:, 0:ny, :], load_sem.at[7]),
    ]
    for copy in small + large:
        copy.start()

    turn = (2, 1, 3, 0)
    depth = n_gy // 4
    near = [lax.rem(lax.rem(gy, 4) + dy, 4) for dy in range(4)]
    far = [lax.rem(lax.div(gy, 4) + dz, depth) * 4 for dz in range(depth)]
    lines = [far[dz] + near[dy] for dz in turn[:depth] for dy in turn if (dz, dy) != (0, 0)]

    def each_peer(do):
        @pl.loop(0, n_gx)
        def _(k):
            x = lax.rem(gx + n_gx // 2 + k, n_gx)
            for y in lines:
                do(x, y)

        for dx in range(1, n_gx):
            do(lax.rem(gx + dx, n_gx), gy)

    barrier = pltpu.get_barrier_semaphore()
    each_peer(lambda x, y: pl.semaphore_signal(barrier, inc=1, device_id=(x, y), device_id_type=MESH))

    for copy in small:
        copy.wait()
    blocks = held // 128
    wide[0:held, :] = prof[...].astype(jnp.float32)
    wide[held:held + CAP, :] = jnp.zeros((CAP, levels), jnp.float32)
    for b in range(blocks):
        table[b, 0:1, :] = lon[b:b + 1, :]
        table[b, 1:2, :] = lat[b:b + 1, :]
        table[b, 2:4, :] = weight[:, b * 128:(b + 1) * 128]
        table[b, 4:8, :] = jnp.zeros((4, 128), jnp.int32)
    for b in range(blocks, blocks + 2):
        table[b] = jnp.zeros((8, 128), jnp.int32)
    lane = lax.broadcasted_iota(jnp.int32, (8, 128), 1)
    field = lax.broadcasted_iota(jnp.int32, (8, 128), 0)

    def one(d, start):
        count = counts[0, d]
        prof_send[d] = wide[pl.ds(start, CAP), :].astype(jnp.bfloat16)
        at = lax.rem(start, 128)
        b = lax.div(start, 128)
        back = lax.rem(128 - at, 128)
        here = pltpu.roll(table[b], back, 1)
        there = pltpu.roll(table[b + 1], back, 1)
        got = jnp.where(lane < 128 - at, here, there)
        got = jnp.where((field == 1) & (lane >= count), unused_lat, got)
        row = jnp.where((field == 0) & (lane < CAP), got, 0)
        for f in range(1, 4):
            moved = pltpu.roll(got, f * CAP, 1)
            row = row + jnp.where((field == f) & (lane >= f * CAP) & (lane < (f + 1) * CAP), moved, 0)
        meta_send[pl.ds(d, 1), :] = jnp.sum(row, axis=0, keepdims=True)
        return start + count

    lax.fori_loop(0, peers, one, jnp.int32(0), unroll=16)

    def remote(src, dst, ssem, rsem, x, y):
        return pltpu.make_async_remote_copy(
            src_ref=src, dst_ref=dst, send_sem=ssem, recv_sem=rsem, device_id=(x, y), device_id_type=MESH)

    has_n = gy < n_gy - 1
    has_s = gy > 0
    up = jnp.minimum(gy + 1, n_gy - 1)
    down = jnp.maximum(gy - 1, 0)
    e = lax.rem(gx + 1, n_gx)
    w = lax.rem(gx + n_gx - 1, n_gx)

    def halo(k, src, dst, x, y):
        return remote(src, dst, hsend.at[k], hrecv.at[k], x, y)

    to_e = halo(0, diff_stage.at[(nx - 1) * pitch:(nx - 1) * pitch + ny], diff_cols.at[0], e, gy)
    to_w = halo(1, diff_stage.at[0:ny], diff_cols.at[1], w, gy)
    to_n = [halo(2, row_stage.at[1], diff_rows.at[1], gx, up),
            halo(3, high_stage.at[1], inv_halo.at[1], gx, up)]
    to_s = [halo(4, row_stage.at[0], diff_rows.at[0], gx, down),
            halo(5, high_stage.at[0], inv_halo.at[0], gx, down)]
    large[0].wait()
    large[1].wait()
    for k, y in ((0, 0), (1, ny - 1)):
        row_stage[k] = diff_stage[pl.ds(y, nx, stride=pitch), :].astype(jnp.bfloat16)
        high_stage[k] = inv_stage[y].astype(jnp.bfloat16)
    pl.semaphore_wait(barrier, peers - 1)

    def send(x, y):
        to = x * n_gy + y
        remote(prof_send.at[to], prof_out.at[me], psend, precv, x, y).start()
        remote(meta_send.at[pl.ds(to, 1)], meta_out.at[pl.ds(me, 1)], msend, mrecv, x, y).start()

    each_peer(send)
    to_e.start()
    to_w.start()

    @pl.when(has_n)
    def _():
        for copy in to_n:
            copy.start()

    @pl.when(has_s)
    def _():
        for copy in to_s:
            copy.start()

    prof_out[me] = prof_send[me]
    meta_out[pl.ds(me, 1), :] = meta_send[pl.ds(me, 1), :]
    empty = jnp.zeros((CLEAR, levels), jnp.float32)

    @pl.loop(0, acc1.shape[0] // CLEAR)
    def _(i):
        rows = pl.ds(pl.multiple_of(i * CLEAR, CLEAR), CLEAR)
        for acc in (acc1, acc2, acc3):
            acc[rows, :] = empty

    @pl.loop(0, ny, unroll=4)
    def _(y):
        inv_out[y] = split(inv_stage[y])

    large[2].wait()
    margin = jnp.zeros((EDGE, levels), jnp.float32)

    @pl.loop(0, ny, unroll=2)
    def _(y):
        first = pl.multiple_of(y * wide_x, 8)
        acc0[pl.ds(first, nx), :] = state_stage[pl.ds(y, nx, stride=pitch), :]
        acc0[pl.ds(first + nx, EDGE), :] = margin
        diff_out[y] = diff_stage[pl.ds(y, nx, stride=pitch), :]

    tail = acc0.shape[0] - ny * wide_x
    acc0[ny * wide_x:, :] = jnp.zeros((tail, levels), jnp.float32)
    n = peers - 1
    whole_p = remote(prof_send.at[0:n], prof_out.at[0:n], psend, precv, gx, gy)
    whole_m = remote(meta_send.at[0:n], meta_out.at[0:n], msend, mrecv, gx, gy)
    whole_p.wait_recv()
    whole_m.wait_recv()
    whole_p.wait_send()
    whole_m.wait_send()
    for copy in (to_e, to_w):
        copy.wait_send()
        copy.wait_recv()

    @pl.when(has_n)
    def _():
        for copy in to_n:
            copy.wait_send()
        for copy in to_s:
            copy.wait_recv()

    @pl.when(has_s)
    def _():
        for copy in to_s:
            copy.wait_send()
        for copy in to_n:
            copy.wait_recv()


def exchange(counts, prof, lon, lat, weight, state, diff, inv, unused_lat, n_gx, n_gy):
    held, levels = prof.shape
    nx, ny, _ = state.shape
    peers = counts.shape[1]
    vm = pltpu.VMEM
    dma = pltpu.SemaphoreType.DMA
    hbm = functools.partial(pltpu.with_memory_space_constraint, memory_space=pltpu.HBM)
    args = (counts, prof, lon.reshape(-1, 128), lat.reshape(-1, 128), weight, state, diff, inv)
    pitched = (nx * (ny + 8), levels)
    rows = -(-(ny + 3) * (nx + EDGE) // CLEAR) * CLEAR
    return pl.pallas_call(
        functools.partial(exchange_body, n_gx, n_gy, unused_lat),
        out_shape=(
            vm((peers, CAP, levels), jnp.bfloat16),
            vm((peers, 128), jnp.int32),
            vm((ny, nx, levels), jnp.float32),
            vm((ny, levels, 2 * levels), jnp.bfloat16),
            vm((2, levels, levels), jnp.bfloat16),
            vm((2, nx, levels), jnp.bfloat16),
            vm((2, ny, levels), jnp.float32),
            *[vm((rows, levels), jnp.float32)] * ACCS,
        ),
        in_specs=[pl.BlockSpec(memory_space=pltpu.HBM)] * 8,
        out_specs=[pl.BlockSpec(memory_space=vm)] * (7 + ACCS),
        scratch_shapes=[
            pltpu.SMEM((1, peers), jnp.int32),
            vm((held, levels), jnp.bfloat16),
            vm((held // 128, 128), jnp.int32),
            vm((held // 128, 128), jnp.int32),
            vm((2, held), jnp.int32),
            vm((held + CAP, levels), jnp.float32),
            vm((held // 128 + 2, 8, 128), jnp.int32),
            vm((peers, CAP, levels), jnp.bfloat16),
            vm((peers, 128), jnp.int32),
            vm((ny, levels, levels), jnp.float32),
            vm(pitched, jnp.float32),
            vm(pitched, jnp.float32),
            vm((2, nx, levels), jnp.bfloat16),
            vm((2, levels, levels), jnp.bfloat16),
            dma((8,)), dma, dma, dma, dma, dma((6,)), dma((6,)),
        ],
        compiler_params=pltpu.CompilerParams(
            collective_id=0, has_side_effects=True, vmem_limit_bytes=17 * 1024 * 1024),
        name="exchange",
    )(*[hbm(a) for a in args])


SLOTS = 64


def scatter_body(nx, ny, prof_ref, meta_ref, *rest):
    peers, cap, levels = prof_ref.shape
    pitch = nx + EDGE
    accs = rest[ACCS:2 * ACCS]
    edge_e, edge_w, edge_n, edge_s, knot, table, index_v, index_s, index_sem = rest[2 * ACCS:]
    meta = meta_ref[...]
    lat_up = pltpu.roll(meta, 128 - cap, 1)
    index_v[...] = lat_up * pitch + meta
    index_copy = pltpu.make_async_copy(index_v, index_s, index_sem)
    index_copy.start()
    group = 8
    lane = lax.broadcasted_iota(jnp.int32, (group, cap, 128), 2)
    slot = lax.broadcasted_iota(jnp.int32, (group, cap, 128), 1)
    own = (lane % cap == slot).astype(jnp.float32)
    r = lax.broadcasted_iota(jnp.int32, (128, 2 * levels), 0) // cap
    c = lax.broadcasted_iota(jnp.int32, (128, 2 * levels), 1) // levels
    pick = (r == c + 2).astype(jnp.bfloat16)

    @pl.loop(0, peers // group, unroll=4)
    def _(i):
        m = meta_ref[pl.ds(pl.multiple_of(i * group, group), group), :].astype(jnp.float32)
        spread = (m[:, None, :] * own).reshape(group * cap, 128).astype(jnp.bfloat16)
        frac = jnp.dot(spread, pick, preferred_element_type=jnp.float32) * (1.0 / SLOTS)
        fx = frac[:, :levels]
        fy = frac[:, levels:]
        p = prof_ref[pl.ds(i * group, group)].reshape(group * cap, levels).astype(jnp.float32)
        p1 = p * fx
        p0 = p - p1
        q01 = p0 * fy
        q11 = p1 * fy
        base = i * (group * cap * 4)
        n = group * cap
        table[pl.ds(base, n, stride=4), :] = p0 - q01
        table[pl.ds(base + 1, n, stride=4), :] = p1 - q11
        table[pl.ds(base + 2, n, stride=4), :] = q01
        table[pl.ds(base + 3, n, stride=4), :] = q11

    index_copy.wait()

    @pl.loop(0, peers)
    def _(s):
        first = pl.multiple_of(s * (cap * 4), cap * 4)
        for k in range(0, cap, ACCS):
            for j in range(ACCS):
                at = index_s[s, k + j]
                row = first + (k + j) * 4
                acc = accs[j]
                acc[pl.ds(at, 2), :] += table[pl.ds(row, 2), :]
                acc[pl.ds(at + pitch, 2), :] += table[pl.ds(row + 2, 2), :]

    def total(at, n):
        out = accs[0][pl.ds(at, n), :]
        for acc in accs[1:]:
            out = out + acc[pl.ds(at, n), :]
        return out

    @pl.loop(0, ny, unroll=8)
    def _(y):
        first = pl.multiple_of(y * pitch, 8)
        edge_w[pl.ds(y, 1), :] = total(first, 8)[0:1]
        edge_e[pl.ds(y, 1), :] = total(first + nx - 8, 8)[7:8]
        edge_e[pl.ds(ny + y, 1), :] = total(first + nx, 8)[0:1]

    edge_s[...] = total(0, nx).astype(edge_s.dtype)
    edge_n[0] = total((ny - 1) * pitch, nx).astype(edge_n.dtype)
    edge_n[1] = total(ny * pitch, nx).astype(edge_n.dtype)
    corner = total(ny * pitch + nx, 8)
    edge_e[2 * ny:2 * ny + 8, :] = corner
    knot[0:1, :] = corner[0:1]
    knot[1:2, :] = total((ny - 1) * pitch + nx, 8)[0:1]
    knot[2:3, :] = total(ny * pitch + nx - 8, 8)[7:8]
    knot[3:4, :] = total(nx, 8)[0:1]
    knot[4:5, :] = total(ny * pitch, 8)[0:1]
    knot[5:8, :] = jnp.zeros((3, levels), jnp.float32)


def scatter(prof, meta, accs, nx, ny):
    peers, cap, levels = prof.shape
    vm = pltpu.VMEM
    block = pl.BlockSpec(memory_space=vm)
    return pl.pallas_call(
        functools.partial(scatter_body, nx, ny),
        out_shape=(
            *[vm(accs[0].shape, jnp.float32)] * ACCS,
            vm((2 * ny + 8, levels), jnp.float32),
            vm((ny, levels), jnp.float32),
            vm((2, nx, levels), jnp.bfloat16),
            vm((nx, levels), jnp.bfloat16),
            vm((8, levels), jnp.float32),
        ),
        in_specs=[block] * (2 + ACCS),
        out_specs=[block] * (5 + ACCS),
        scratch_shapes=[
            vm((peers * cap * 4 + 8, levels), jnp.float32),
            vm((peers, 128), jnp.int32),
            pltpu.SMEM((peers, 128), jnp.int32),
            pltpu.SemaphoreType.DMA,
        ],
        input_output_aliases={2 + k: k for k in range(ACCS)},
        compiler_params=pltpu.CompilerParams(vmem_limit_bytes=5 * 1024 * 1024),
        name="scatter",
    )(prof, meta, *accs)


STEPS = 4
CHUNK = 16


def steps_body(n_gx, n_gy, acc0, acc1, acc2, acc3, edge_e, edge_w, edge_n, edge_s, knot,
               diff_ref, inv_pair, inv_halo, diff_rows, diff_cols, out_ref,
               mu_ref, g_last, g_other, col_send, col_recv, row_send, row_recv, in_w, in_e, in_s, in_n, knots,
               spill_send, spill_recv, col_ssem, col_rsem, row_ssem, row_rsem):
    ny, nx, levels = diff_ref.shape
    pitch = nx + EDGE
    gx = lax.axis_index("gx")
    gy = lax.axis_index("gy")
    e = lax.rem(gx + 1, n_gx)
    w = lax.rem(gx + n_gx - 1, n_gx)
    has_n = gy < n_gy - 1
    has_s = gy > 0
    up = jnp.minimum(gy + 1, n_gy - 1)
    down = jnp.maximum(gy - 1, 0)
    barrier = pltpu.get_barrier_semaphore()

    def greet(x, y):
        pl.semaphore_signal(barrier, inc=1, device_id=(x, y), device_id_type=MESH)

    greet(e, gy)
    greet(w, gy)

    @pl.when(has_n)
    def _():
        greet(gx, up)
        greet(e, up)
        greet(w, up)

    @pl.when(has_s)
    def _():
        greet(gx, down)
        greet(e, down)
        greet(w, down)

    pl.semaphore_wait(barrier, 2 + 3 * has_n.astype(jnp.int32) + 3 * has_s.astype(jnp.int32))

    def remote(src, dst, ssem, rsem, x, y):
        return pltpu.make_async_remote_copy(
            src_ref=src, dst_ref=dst, send_sem=ssem, recv_sem=rsem, device_id=(x, y), device_id_type=MESH)

    def spill(k, src, dst, x, y):
        return remote(src, dst, spill_send.at[k], spill_recv.at[k], x, y)

    across = [spill(0, edge_e, in_w, e, gy), spill(1, edge_w, in_e, w, gy)]
    north_to = [spill(2, edge_n, in_s, gx, up), spill(4, knot, knots.at[0], e, up),
                spill(6, knot, knots.at[2], w, up), spill(7, knot, knots.at[3], gx, up)]
    south_to = [spill(3, edge_s, in_n, gx, down), spill(5, knot, knots.at[1], e, down)]
    for copy in across:
        copy.start()

    @pl.when(has_n)
    def _():
        for copy in north_to:
            copy.start()

    @pl.when(has_s)
    def _():
        for copy in south_to:
            copy.start()

    zeros = jnp.zeros((nx + 2 * EDGE, levels), jnp.float32)

    @pl.when(jnp.logical_not(has_s))
    def _():
        g_other[0] = zeros
        g_last[0] = zeros

    @pl.when(jnp.logical_not(has_n))
    def _():
        g_other[ny + 1] = zeros
        g_last[ny + 1] = zeros

    chunks = ny // CHUNK

    def cols(n, side, c):
        rows = pl.ds(pl.multiple_of(c * CHUNK, CHUNK), CHUNK)
        return remote(col_send.at[n, side, rows], col_recv.at[n, side, rows],
                      col_ssem.at[n, side, c], col_rsem.at[n, side, c], e if side == 0 else w, gy)

    def flux(n):
        return g_last if (STEPS - 1 - n) % 2 == 0 else g_other

    def rowcopy(n, side):
        return remote(row_send.at[n, side], row_recv.at[n, side],
                      row_ssem.at[n, side], row_rsem.at[n, side], gx, up if side == 0 else down)

    def stencil(g, y):
        mid = g[y + 1, pl.ds(EDGE, nx), :]
        near = (g[y + 1, pl.ds(EDGE - 1, nx), :] + g[y + 1, pl.ds(EDGE + 1, nx), :]) + (
            g[y, pl.ds(EDGE, nx), :] + g[y + 2, pl.ds(EDGE, nx), :])
        return mu_ref[y] + (near - 4.0 * mid)

    first_lane = lax.broadcasted_iota(jnp.int32, (8, levels), 0) == 0

    side_lane = lax.broadcasted_iota(jnp.int32, (16, levels), 0)

    def sides(y):
        spilled = in_w[pl.ds(ny + y, 1), :]
        west = in_w[pl.ds(y, 1), :]
        east = in_e[pl.ds(y, 1), :] + edge_e[pl.ds(ny + y, 1), :]
        lam = jnp.where(side_lane == 0, spilled, jnp.where(side_lane == 1, west, jnp.where(side_lane == 2, east, 0.0)))
        mu = jnp.dot(lam.astype(jnp.bfloat16), inv_pair[y, :, 0:levels], preferred_element_type=jnp.float32)
        g = flux(0)
        mu_ref[y, 0:1, :] += mu[0:1]
        g[y + 1, EDGE:EDGE + 1, :] += diff_ref[y, 0:1, :] * mu[0:1]
        g[y + 1, EDGE - 1:EDGE, :] = diff_cols[0, pl.ds(y, 1), :] * mu[1:2]
        g[y + 1, EDGE + nx:EDGE + nx + 1, :] = diff_cols[1, pl.ds(y, 1), :] * mu[2:3]

    def beside(lam, extra):
        head = lam[0:8] + jnp.where(first_lane, extra, 0.0)
        return jnp.concatenate([head, lam[8:]], axis=0).astype(jnp.bfloat16)

    def mixed(lam, y):
        pair = inv_pair[y]
        both = jnp.dot(split(lam), jnp.concatenate([pair, pair], axis=0), preferred_element_type=jnp.float32)
        mu = both[:, :levels] + both[:, levels:]
        return mu, diff_ref[y] * mu

    def neighbours_in():
        @pl.when(has_s)
        def _():
            for copy in north_to:
                copy.wait_recv()
            fresh, g = mixed(in_s[1].astype(jnp.float32), 0)
            mu_ref[0] += fresh
            flux(0)[1, EDGE:EDGE + nx, :] += g
            in_w[ny:ny + 1, :] += knots[0, 0:1, :]
            in_w[0:1, :] += knots[0, 2:3, :]
            in_e[0:1, :] += knots[2, 4:5, :] + knots[3, 0:1, :]
            lam = beside(in_s[0].astype(jnp.float32), knots[0, 1:2, :])
            mu = jnp.dot(lam, inv_halo[1], preferred_element_type=jnp.float32)
            flux(0)[0, EDGE:EDGE + nx, :] = diff_rows[1].astype(jnp.float32) * mu

        @pl.when(has_n)
        def _():
            for copy in south_to:
                copy.wait_recv()
            lam = beside(in_n[...].astype(jnp.float32) + edge_n[1].astype(jnp.float32),
                         knots[1, 3:4, :] + in_w[2 * ny:2 * ny + 1, :])
            mu = jnp.dot(lam, inv_halo[0], preferred_element_type=jnp.float32)
            flux(0)[ny + 1, EDGE:EDGE + nx, :] = diff_rows[0].astype(jnp.float32) * mu

    def row(n, y):
        if n > 0:
            return mixed(stencil(flux(n - 1), y), y)
        rows = pl.ds(pl.multiple_of(y * pitch, 8), nx)
        return mixed((acc0[rows, :] + acc1[rows, :]) + (acc2[rows, :] + acc3[rows, :]), y)

    def columns_in(n, c):
        for side in range(2):
            cols(n, side, c).wait_recv()
        for r in range(CHUNK):
            y = c * CHUNK + r
            flux(n)[y + 1, EDGE - 1:EDGE, :] = col_recv[n, 0, pl.ds(y, 1), :]
            flux(n)[y + 1, EDGE + nx:EDGE + nx + 1, :] = col_recv[n, 1, pl.ds(y, 1), :]

    def rows_in(n):
        @pl.when(has_s)
        def _():
            rowcopy(n, 0).wait_recv()
            flux(n)[0, EDGE:EDGE + nx, :] = row_recv[n, 0].astype(jnp.float32)

        @pl.when(has_n)
        def _():
            rowcopy(n, 1).wait_recv()
            flux(n)[ny + 1, EDGE:EDGE + nx, :] = row_recv[n, 1].astype(jnp.float32)

    def north_out(n):
        @pl.when(has_n)
        def _():
            rowcopy(n, 0).start()

    def south_out(n):
        @pl.when(has_s)
        def _():
            rowcopy(n, 1).start()

    for n in range(STEPS):
        if n > 0:
            if n > 1:
                columns_in(n - 1, chunks - 1)
                columns_in(n - 1, 0)
                rows_in(n - 1)
            row_send[n, 0] = row(n, ny - 1)[1].astype(row_send.dtype)
            row_send[n, 1] = row(n, 0)[1].astype(row_send.dtype)
            north_out(n)
            south_out(n)

        @pl.loop(0, chunks)
        def _(i):
            c = lax.rem(i + chunks - 1, chunks)
            if n > 1:

                @pl.when(i > 1)
                def _():
                    columns_in(n - 1, c)

            for r in range(CHUNK):
                y = c * CHUNK + r
                mu, g = row(n, y)
                mu_ref[y] = mu
                flux(n)[y + 1, pl.ds(EDGE, nx), :] = g
                if n > 0:
                    col_send[n, 0, pl.ds(y, 1), :] = g[nx - 1:nx]
                    col_send[n, 1, pl.ds(y, 1), :] = g[0:1]

            if n > 0:
                for side in range(2):
                    cols(n, side, c).start()

        if n == 0:
            for copy in across:
                copy.wait_recv()

            @pl.loop(0, chunks)
            def _(i):
                c = chunks - 1 - i
                pl.when(i == chunks - 1)(neighbours_in)
                for r in range(CHUNK):
                    sides(c * CHUNK + r)

    last = STEPS - 1

    out_pitch = out_ref.shape[0] // nx
    nothing = jnp.zeros((1, levels), jnp.float32)
    g_last[0] = zeros
    g_last[ny + 1] = zeros

    @pl.loop(0, chunks)
    def _(c):
        for r in range(CHUNK):
            y = c * CHUNK + r
            g_last[y + 1, EDGE - 1:EDGE, :] = nothing
            g_last[y + 1, EDGE + nx:EDGE + nx + 1, :] = nothing

    @pl.loop(0, chunks)
    def _(c):
        for r in range(CHUNK):
            y = c * CHUNK + r
            out_ref[pl.ds(y, nx, stride=out_pitch), :] = stencil(g_last, y)

    @pl.loop(0, chunks)
    def _(c):
        for side in range(2):
            cols(last, side, c).wait_recv()

    east_edge = (nx - 1) * out_pitch
    out_ref[0:ny, :] += col_recv[last, 0]
    out_ref[east_edge:east_edge + ny, :] += col_recv[last, 1]

    @pl.when(has_s)
    def _():
        rowcopy(last, 0).wait_recv()
        out_ref[pl.ds(0, nx, stride=out_pitch), :] += row_recv[last, 0].astype(jnp.float32)

    @pl.when(has_n)
    def _():
        rowcopy(last, 1).wait_recv()
        out_ref[pl.ds(ny - 1, nx, stride=out_pitch), :] += row_recv[last, 1].astype(jnp.float32)

    @pl.when(has_s)
    def _():
        for n in range(1, STEPS):
            rowcopy(n, 1).wait_send()
        for copy in south_to:
            copy.wait_send()

    @pl.when(has_n)
    def _():
        for n in range(1, STEPS):
            rowcopy(n, 0).wait_send()
        for copy in north_to:
            copy.wait_send()

    for copy in across:
        copy.wait_send()
    for n in range(1, STEPS):

        @pl.loop(0, chunks)
        def _(c):
            for side in range(2):
                cols(n, side, c).wait_send()


def steps(accs, edges, diffusion, inverse, halos, n_gx, n_gy, space=None):
    ny, nx, levels = diffusion.shape
    vm = pltpu.VMEM
    chunks = ny // CHUNK
    dma = pltpu.SemaphoreType.DMA
    make = space or (lambda s, d: jax.ShapeDtypeStruct(s, d))
    return pl.pallas_call(
        functools.partial(steps_body, n_gx, n_gy),
        out_shape=make((nx * (ny + 8), levels), jnp.float32),
        in_specs=[pl.BlockSpec(memory_space=vm)] * (10 + ACCS),
        out_specs=pl.BlockSpec(memory_space=vm),
        scratch_shapes=[
            vm((ny, nx, levels), jnp.float32),
            vm((ny + 2, nx + 2 * EDGE, levels), jnp.float32),
            vm((ny + 2, nx + 2 * EDGE, levels), jnp.float32),
            vm((STEPS, 2, ny, levels), jnp.float32),
            vm((STEPS, 2, ny, levels), jnp.float32),
            vm((STEPS, 2, nx, levels), jnp.bfloat16),
            vm((STEPS, 2, nx, levels), jnp.bfloat16),
            vm((2 * ny + 8, levels), jnp.float32),
            vm((ny, levels), jnp.float32),
            vm((2, nx, levels), jnp.bfloat16),
            vm((nx, levels), jnp.bfloat16),
            vm((4, 8, levels), jnp.float32),
            dma((8,)), dma((8,)),
            dma((STEPS, 2, chunks)), dma((STEPS, 2, chunks)), dma((STEPS, 2)), dma((STEPS, 2)),
        ],
        compiler_params=pltpu.CompilerParams(
            collective_id=1, has_side_effects=True, vmem_limit_bytes=17 * 1024 * 1024),
        name="steps",
    )(*accs, *edges, diffusion, inverse, *halos)


def finish_body(parts, stage, out_ref, sems):
    nx, ny, levels = out_ref.shape
    wide = stage.reshape(nx, stage.shape[0] // nx, levels)
    step = nx // parts
    copies = [
        pltpu.make_async_copy(wide.at[k * step:(k + 1) * step, 0:ny, :], out_ref.at[k * step:(k + 1) * step], sems.at[k])
        for k in range(parts)
    ]
    for copy in copies:
        copy.start()
    for copy in copies:
        copy.wait()


def finish(stage, nx, ny):
    levels = stage.shape[1]
    parts = 8
    return pl.pallas_call(
        functools.partial(finish_body, parts),
        out_shape=jax.ShapeDtypeStruct((nx, ny, levels), jnp.float32),
        in_specs=[pl.BlockSpec(memory_space=pltpu.VMEM)],
        out_specs=pl.BlockSpec(memory_space=pltpu.HBM),
        scratch_shapes=[pltpu.SemaphoreType.DMA((parts,))],
        compiler_params=pltpu.CompilerParams(vmem_limit_bytes=1024 * 1024),
        name="finish",
    )(stage)


def shards(n_gx, n_gy, state, diffusion, vert_inverse, profiles, counts, cell_lon, cell_lat, weight_slot):
    nx, ny, _ = state.shape
    got, got_meta, diffusion, inverse, *rest = exchange(
        counts, profiles, cell_lon, cell_lat, weight_slot, state, diffusion, vert_inverse, ny + 1, n_gx, n_gy)
    made = scatter(got, got_meta, rest[3:], nx, ny)
    stage = steps(made[:ACCS], made[ACCS:], diffusion, inverse, rest[:3], n_gx, n_gy, pltpu.VMEM)
    return finish(stage, nx, ny)


def solution(mesh):
    return jax.shard_map(
        functools.partial(shards, mesh.shape["gx"], mesh.shape["gy"]),
        mesh=mesh,
        in_specs=(
            P("gx", "gy", None),
            P("gx", "gy", None),
            P("gy", None, None),
            P(("gx", "gy"), None),
            P(("gx", "gy"), None),
            P(("gx", "gy")),
            P(("gx", "gy")),
            P(None, ("gx", "gy")),
        ),
        out_specs=P("gx", "gy", None),
        check_vma=False,
    )
```

```python
import functools

import jax
import jax.numpy as jnp
from jax import lax
from jax.experimental import pallas as pl
from jax.experimental.pallas import tpu as pltpu
from jax.sharding import PartitionSpec as P

CAP = 16
MESH = pl.DeviceIdType.MESH

ACCS = 4
EDGE = 8
CLEAR = 64


def split(value):
    high = value.astype(jnp.bfloat16)
    low = (value - high.astype(jnp.float32)).astype(jnp.bfloat16)
    return jnp.concatenate([high, low], axis=1)


def exchange_body(n_gx, n_gy, unused_lat, counts_ref, prof_ref, lon_ref, lat_ref, weight_ref, state_ref, diff_ref,
                  inv_ref, prof_out, meta_out, diff_out, inv_out, inv_halo, diff_rows, diff_cols, acc0, acc1, acc2, acc3,
                  counts, prof, lon, lat, weight, wide, table, prof_send, meta_send, inv_stage, state_stage, diff_stage, row_stage, high_stage,
                  load_sem, psend, precv, msend, mrecv, hsend, hrecv):
    held, levels = prof_ref.shape
    peers = prof_out.shape[0]
    nx, ny, _ = state_ref.shape
    pitch = state_stage.shape[0] // nx
    wide_x = nx + EDGE
    gx = lax.axis_index("gx")
    gy = lax.axis_index("gy")
    me = gx * n_gy + gy
    small = [
        pltpu.make_async_copy(src, dst, load_sem.at[k])
        for k, (src, dst) in enumerate(
            [(counts_ref, counts), (prof_ref, prof), (lon_ref, lon), (lat_ref, lat), (weight_ref, weight)])
    ]
    large = [
        pltpu.make_async_copy(diff_ref, diff_stage.reshape(nx, pitch, levels).at[:, 0:ny, :], load_sem.at[5]),
        pltpu.make_async_copy(inv_ref, inv_stage, load_sem.at[6]),
        pltpu.make_async_copy(state_ref, state_stage.reshape(nx, pitch, levels).at[:, 0:ny, :], load_sem.at[7]),
    ]
    for copy in small:
        copy.start()

    turn = (2, 1, 3, 0)
    depth = n_gy // 4
    near = [lax.rem(lax.rem(gy, 4) + dy, 4) for dy in range(4)]
    far = [lax.rem(lax.div(gy, 4) + dz, depth) * 4 for dz in range(depth)]
    lines = [far[dz] + near[dy] for dz in turn[:depth] for dy in turn if (dz, dy) != (0, 0)]

    def each_peer(do):
        @pl.loop(0, n_gx)
        def _(k):
            x = lax.rem(gx + n_gx // 2 + k, n_gx)
            for y in lines:
                do(x, y)

        for dx in range(1, n_gx):
            do(lax.rem(gx + dx, n_gx), gy)

    barrier = pltpu.get_barrier_semaphore()
    each_peer(lambda x, y: pl.semaphore_signal(barrier, inc=1, device_id=(x, y), device_id_type=MESH))

    for copy in small:
        copy.wait()
    for copy in large:
        copy.start()
    blocks = held // 128
    wide[0:held, :] = prof[...].astype(jnp.float32)
    wide[held:held + CAP, :] = jnp.zeros((CAP, levels), jnp.float32)
    for b in range(blocks):
        table[b, 0:1, :] = lon[b:b + 1, :]
        table[b, 1:2, :] = lat[b:b + 1, :]
        table[b, 2:4, :] = weight[:, b * 128:(b + 1) * 128]
        table[b, 4:8, :] = jnp.zeros((4, 128), jnp.int32)
    for b in range(blocks, blocks + 2):
        table[b] = jnp.zeros((8, 128), jnp.int32)
    lane = lax.broadcasted_iota(jnp.int32, (8, 128), 1)
    field = lax.broadcasted_iota(jnp.int32, (8, 128), 0)

    def one(d, start):
        count = counts[0, d]
        prof_send[d] = wide[pl.ds(start, CAP), :].astype(jnp.bfloat16)
        at = lax.rem(start, 128)
        b = lax.div(start, 128)
        back = lax.rem(128 - at, 128)
        here = pltpu.roll(table[b], back, 1)
        there = pltpu.roll(table[b + 1], back, 1)
        got = jnp.where(lane < 128 - at, here, there)
        got = jnp.where((field == 1) & (lane >= count), unused_lat, got)
        row = jnp.where((field == 0) & (lane < CAP), got, 0)
        for f in range(1, 4):
            moved = pltpu.roll(got, f * CAP, 1)
            row = row + jnp.where((field == f) & (lane >= f * CAP) & (lane < (f + 1) * CAP), moved, 0)
        meta_send[pl.ds(d, 1), :] = jnp.sum(row, axis=0, keepdims=True)
        return start + count

    lax.fori_loop(0, peers, one, jnp.int32(0), unroll=16)

    def remote(src, dst, ssem, rsem, x, y):
        return pltpu.make_async_remote_copy(
            src_ref=src, dst_ref=dst, send_sem=ssem, recv_sem=rsem, device_id=(x, y), device_id_type=MESH)

    has_n = gy < n_gy - 1
    has_s = gy > 0
    up = jnp.minimum(gy + 1, n_gy - 1)
    down = jnp.maximum(gy - 1, 0)
    e = lax.rem(gx + 1, n_gx)
    w = lax.rem(gx + n_gx - 1, n_gx)

    def halo(k, src, dst, x, y):
        return remote(src, dst, hsend.at[k], hrecv.at[k], x, y)

    to_e = halo(0, diff_stage.at[(nx - 1) * pitch:(nx - 1) * pitch + ny], diff_cols.at[0], e, gy)
    to_w = halo(1, diff_stage.at[0:ny], diff_cols.at[1], w, gy)
    to_n = [halo(2, row_stage.at[1], diff_rows.at[1], gx, up),
            halo(3, high_stage.at[1], inv_halo.at[1], gx, up)]
    to_s = [halo(4, row_stage.at[0], diff_rows.at[0], gx, down),
            halo(5, high_stage.at[0], inv_halo.at[0], gx, down)]
    pl.semaphore_wait(barrier, peers - 1)

    def send(x, y):
        to = x * n_gy + y
        remote(prof_send.at[to], prof_out.at[me], psend, precv, x, y).start()
        remote(meta_send.at[pl.ds(to, 1)], meta_out.at[pl.ds(me, 1)], msend, mrecv, x, y).start()

    each_peer(send)
    large[0].wait()
    large[1].wait()
    for k, y in ((0, 0), (1, ny - 1)):
        row_stage[k] = diff_stage[pl.ds(y, nx, stride=pitch), :].astype(jnp.bfloat16)
        high_stage[k] = inv_stage[y].astype(jnp.bfloat16)
    to_e.start()
    to_w.start()

    @pl.when(has_n)
    def _():
        for copy in to_n:
            copy.start()

    @pl.when(has_s)
    def _():
        for copy in to_s:
            copy.start()

    prof_out[me] = prof_send[me]
    meta_out[pl.ds(me, 1), :] = meta_send[pl.ds(me, 1), :]
    empty = jnp.zeros((CLEAR, levels), jnp.float32)

    @pl.loop(0, acc1.shape[0] // CLEAR)
    def _(i):
        rows = pl.ds(pl.multiple_of(i * CLEAR, CLEAR), CLEAR)
        for acc in (acc1, acc2, acc3):
            acc[rows, :] = empty

    @pl.loop(0, ny, unroll=4)
    def _(y):
        inv_out[y] = split(inv_stage[y])

    large[2].wait()
    margin = jnp.zeros((EDGE, levels), jnp.float32)

    @pl.loop(0, ny, unroll=2)
    def _(y):
        first = pl.multiple_of(y * wide_x, 8)
        acc0[pl.ds(first, nx), :] = state_stage[pl.ds(y, nx, stride=pitch), :]
        acc0[pl.ds(first + nx, EDGE), :] = margin
        diff_out[y] = diff_stage[pl.ds(y, nx, stride=pitch), :]

    tail = acc0.shape[0] - ny * wide_x
    acc0[ny * wide_x:, :] = jnp.zeros((tail, levels), jnp.float32)
    n = peers - 1
    whole_p = remote(prof_send.at[0:n], prof_out.at[0:n], psend, precv, gx, gy)
    whole_m = remote(meta_send.at[0:n], meta_out.at[0:n], msend, mrecv, gx, gy)
    whole_p.wait_recv()
    whole_m.wait_recv()
    whole_p.wait_send()
    whole_m.wait_send()
    for copy in (to_e, to_w):
        copy.wait_send()
        copy.wait_recv()

    @pl.when(has_n)
    def _():
        for copy in to_n:
            copy.wait_send()
        for copy in to_s:
            copy.wait_recv()

    @pl.when(has_s)
    def _():
        for copy in to_s:
            copy.wait_send()
        for copy in to_n:
            copy.wait_recv()


def exchange(counts, prof, lon, lat, weight, state, diff, inv, unused_lat, n_gx, n_gy):
    held, levels = prof.shape
    nx, ny, _ = state.shape
    peers = counts.shape[1]
    vm = pltpu.VMEM
    dma = pltpu.SemaphoreType.DMA
    hbm = functools.partial(pltpu.with_memory_space_constraint, memory_space=pltpu.HBM)
    args = (counts, prof, lon.reshape(-1, 128), lat.reshape(-1, 128), weight, state, diff, inv)
    pitched = (nx * (ny + 8), levels)
    rows = -(-(ny + 3) * (nx + EDGE) // CLEAR) * CLEAR
    return pl.pallas_call(
        functools.partial(exchange_body, n_gx, n_gy, unused_lat),
        out_shape=(
            vm((peers, CAP, levels), jnp.bfloat16),
            vm((peers, 128), jnp.int32),
            vm((ny, nx, levels), jnp.float32),
            vm((ny, levels, 2 * levels), jnp.bfloat16),
            vm((2, levels, levels), jnp.bfloat16),
            vm((2, nx, levels), jnp.bfloat16),
            vm((2, ny, levels), jnp.float32),
            *[vm((rows, levels), jnp.float32)] * ACCS,
        ),
        in_specs=[pl.BlockSpec(memory_space=pltpu.HBM)] * 8,
        out_specs=[pl.BlockSpec(memory_space=vm)] * (7 + ACCS),
        scratch_shapes=[
            pltpu.SMEM((1, peers), jnp.int32),
            vm((held, levels), jnp.bfloat16),
            vm((held // 128, 128), jnp.int32),
            vm((held // 128, 128), jnp.int32),
            vm((2, held), jnp.int32),
            vm((held + CAP, levels), jnp.float32),
            vm((held // 128 + 2, 8, 128), jnp.int32),
            vm((peers, CAP, levels), jnp.bfloat16),
            vm((peers, 128), jnp.int32),
            vm((ny, levels, levels), jnp.float32),
            vm(pitched, jnp.float32),
            vm(pitched, jnp.float32),
            vm((2, nx, levels), jnp.bfloat16),
            vm((2, levels, levels), jnp.bfloat16),
            dma((8,)), dma, dma, dma, dma, dma((6,)), dma((6,)),
        ],
        compiler_params=pltpu.CompilerParams(
            collective_id=0, has_side_effects=True, vmem_limit_bytes=17 * 1024 * 1024),
        name="exchange",
    )(*[hbm(a) for a in args])


SLOTS = 64


def scatter_body(nx, ny, prof_ref, meta_ref, *rest):
    peers, cap, levels = prof_ref.shape
    pitch = nx + EDGE
    accs = rest[ACCS:2 * ACCS]
    edge_e, edge_w, edge_n, edge_s, knot, table, index_v, index_s, index_sem = rest[2 * ACCS:]
    meta = meta_ref[...]
    lat_up = pltpu.roll(meta, 128 - cap, 1)
    index_v[...] = lat_up * pitch + meta
    index_copy = pltpu.make_async_copy(index_v, index_s, index_sem)
    index_copy.start()
    group = 8
    lane = lax.broadcasted_iota(jnp.int32, (group, cap, 128), 2)
    slot = lax.broadcasted_iota(jnp.int32, (group, cap, 128), 1)
    own = (lane % cap == slot).astype(jnp.float32)
    r = lax.broadcasted_iota(jnp.int32, (128, 2 * levels), 0) // cap
    c = lax.broadcasted_iota(jnp.int32, (128, 2 * levels), 1) // levels
    pick = (r == c + 2).astype(jnp.bfloat16)

    @pl.loop(0, peers // group, unroll=4)
    def _(i):
        m = meta_ref[pl.ds(pl.multiple_of(i * group, group), group), :].astype(jnp.float32)
        spread = (m[:, None, :] * own).reshape(group * cap, 128).astype(jnp.bfloat16)
        frac = jnp.dot(spread, pick, preferred_element_type=jnp.float32) * (1.0 / SLOTS)
        fx = frac[:, :levels]
        fy = frac[:, levels:]
        p = prof_ref[pl.ds(i * group, group)].reshape(group * cap, levels).astype(jnp.float32)
        p1 = p * fx
        p0 = p - p1
        q01 = p0 * fy
        q11 = p1 * fy
        base = i * (group * cap * 4)
        n = group * cap
        table[pl.ds(base, n, stride=4), :] = p0 - q01
        table[pl.ds(base + 1, n, stride=4), :] = p1 - q11
        table[pl.ds(base + 2, n, stride=4), :] = q01
        table[pl.ds(base + 3, n, stride=4), :] = q11

    index_copy.wait()

    @pl.loop(0, peers)
    def _(s):
        first = pl.multiple_of(s * (cap * 4), cap * 4)
        for k in range(0, cap, ACCS):
            for j in range(ACCS):
                at = index_s[s, k + j]
                row = first + (k + j) * 4
                acc = accs[j]
                acc[pl.ds(at, 2), :] += table[pl.ds(row, 2), :]
                acc[pl.ds(at + pitch, 2), :] += table[pl.ds(row + 2, 2), :]

    def total(at, n):
        out = accs[0][pl.ds(at, n), :]
        for acc in accs[1:]:
            out = out + acc[pl.ds(at, n), :]
        return out

    @pl.loop(0, ny, unroll=8)
    def _(y):
        first = pl.multiple_of(y * pitch, 8)
        edge_w[pl.ds(y, 1), :] = total(first, 8)[0:1]
        edge_e[pl.ds(y, 1), :] = total(first + nx - 8, 8)[7:8]
        edge_e[pl.ds(ny + y, 1), :] = total(first + nx, 8)[0:1]

    edge_s[...] = total(0, nx).astype(edge_s.dtype)
    edge_n[0] = total((ny - 1) * pitch, nx).astype(edge_n.dtype)
    edge_n[1] = total(ny * pitch, nx).astype(edge_n.dtype)
    corner = total(ny * pitch + nx, 8)
    edge_e[2 * ny:2 * ny + 8, :] = corner
    knot[0:1, :] = corner[0:1]
    knot[1:2, :] = total((ny - 1) * pitch + nx, 8)[0:1]
    knot[2:3, :] = total(ny * pitch + nx - 8, 8)[7:8]
    knot[3:4, :] = total(nx, 8)[0:1]
    knot[4:5, :] = total(ny * pitch, 8)[0:1]
    knot[5:8, :] = jnp.zeros((3, levels), jnp.float32)


def scatter(prof, meta, accs, nx, ny):
    peers, cap, levels = prof.shape
    vm = pltpu.VMEM
    block = pl.BlockSpec(memory_space=vm)
    return pl.pallas_call(
        functools.partial(scatter_body, nx, ny),
        out_shape=(
            *[vm(accs[0].shape, jnp.float32)] * ACCS,
            vm((2 * ny + 8, levels), jnp.float32),
            vm((ny, levels), jnp.float32),
            vm((2, nx, levels), jnp.bfloat16),
            vm((nx, levels), jnp.bfloat16),
            vm((8, levels), jnp.float32),
        ),
        in_specs=[block] * (2 + ACCS),
        out_specs=[block] * (5 + ACCS),
        scratch_shapes=[
            vm((peers * cap * 4 + 8, levels), jnp.float32),
            vm((peers, 128), jnp.int32),
            pltpu.SMEM((peers, 128), jnp.int32),
            pltpu.SemaphoreType.DMA,
        ],
        input_output_aliases={2 + k: k for k in range(ACCS)},
        compiler_params=pltpu.CompilerParams(vmem_limit_bytes=5 * 1024 * 1024),
        name="scatter",
    )(prof, meta, *accs)


STEPS = 4
CHUNK = 16


def steps_body(n_gx, n_gy, acc0, acc1, acc2, acc3, edge_e, edge_w, edge_n, edge_s, knot,
               diff_ref, inv_pair, inv_halo, diff_rows, diff_cols, out_ref,
               mu_ref, g_last, g_other, col_send, col_recv, row_send, row_recv, in_w, in_e, in_s, in_n, knots,
               spill_send, spill_recv, col_ssem, col_rsem, row_ssem, row_rsem):
    ny, nx, levels = diff_ref.shape
    pitch = nx + EDGE
    gx = lax.axis_index("gx")
    gy = lax.axis_index("gy")
    e = lax.rem(gx + 1, n_gx)
    w = lax.rem(gx + n_gx - 1, n_gx)
    has_n = gy < n_gy - 1
    has_s = gy > 0
    up = jnp.minimum(gy + 1, n_gy - 1)
    down = jnp.maximum(gy - 1, 0)
    barrier = pltpu.get_barrier_semaphore()

    def greet(x, y):
        pl.semaphore_signal(barrier, inc=1, device_id=(x, y), device_id_type=MESH)

    greet(e, gy)
    greet(w, gy)

    @pl.when(has_n)
    def _():
        greet(gx, up)
        greet(e, up)
        greet(w, up)

    @pl.when(has_s)
    def _():
        greet(gx, down)
        greet(e, down)
        greet(w, down)

    pl.semaphore_wait(barrier, 2 + 3 * has_n.astype(jnp.int32) + 3 * has_s.astype(jnp.int32))

    def remote(src, dst, ssem, rsem, x, y):
        return pltpu.make_async_remote_copy(
            src_ref=src, dst_ref=dst, send_sem=ssem, recv_sem=rsem, device_id=(x, y), device_id_type=MESH)

    def spill(k, src, dst, x, y):
        return remote(src, dst, spill_send.at[k], spill_recv.at[k], x, y)

    across = [spill(0, edge_e, in_w, e, gy), spill(1, edge_w, in_e, w, gy)]
    north_to = [spill(2, edge_n, in_s, gx, up), spill(4, knot, knots.at[0], e, up),
                spill(6, knot, knots.at[2], w, up), spill(7, knot, knots.at[3], gx, up)]
    south_to = [spill(3, edge_s, in_n, gx, down), spill(5, knot, knots.at[1], e, down)]
    for copy in across:
        copy.start()

    @pl.when(has_n)
    def _():
        for copy in north_to:
            copy.start()

    @pl.when(has_s)
    def _():
        for copy in south_to:
            copy.start()

    zeros = jnp.zeros((nx + 2 * EDGE, levels), jnp.float32)

    @pl.when(jnp.logical_not(has_s))
    def _():
        g_other[0] = zeros
        g_last[0] = zeros

    @pl.when(jnp.logical_not(has_n))
    def _():
        g_other[ny + 1] = zeros
        g_last[ny + 1] = zeros

    chunks = ny // CHUNK

    def cols(n, side, c):
        rows = pl.ds(pl.multiple_of(c * CHUNK, CHUNK), CHUNK)
        return remote(col_send.at[n, side, rows], col_recv.at[n, side, rows],
                      col_ssem.at[n, side, c], col_rsem.at[n, side, c], e if side == 0 else w, gy)

    def flux(n):
        return g_last if (STEPS - 1 - n) % 2 == 0 else g_other

    def rowcopy(n, side):
        return remote(row_send.at[n, side], row_recv.at[n, side],
                      row_ssem.at[n, side], row_rsem.at[n, side], gx, up if side == 0 else down)

    def stencil(g, y):
        mid = g[y + 1, pl.ds(EDGE, nx), :]
        near = (g[y + 1, pl.ds(EDGE - 1, nx), :] + g[y + 1, pl.ds(EDGE + 1, nx), :]) + (
            g[y, pl.ds(EDGE, nx), :] + g[y + 2, pl.ds(EDGE, nx), :])
        return mu_ref[y] + (near - 4.0 * mid)

    first_lane = lax.broadcasted_iota(jnp.int32, (8, levels), 0) == 0

    side_lane = lax.broadcasted_iota(jnp.int32, (16, levels), 0)

    def sides(y):
        spilled = in_w[pl.ds(ny + y, 1), :]
        west = in_w[pl.ds(y, 1), :]
        east = in_e[pl.ds(y, 1), :] + edge_e[pl.ds(ny + y, 1), :]
        lam = jnp.where(side_lane == 0, spilled, jnp.where(side_lane == 1, west, jnp.where(side_lane == 2, east, 0.0)))
        mu = jnp.dot(lam.astype(jnp.bfloat16), inv_pair[y, :, 0:levels], preferred_element_type=jnp.float32)
        g = flux(0)
        mu_ref[y, 0:1, :] += mu[0:1]
        g[y + 1, EDGE:EDGE + 1, :] += diff_ref[y, 0:1, :] * mu[0:1]
        g[y + 1, EDGE - 1:EDGE, :] = diff_cols[0, pl.ds(y, 1), :] * mu[1:2]
        g[y + 1, EDGE + nx:EDGE + nx + 1, :] = diff_cols[1, pl.ds(y, 1), :] * mu[2:3]

    def beside(lam, extra):
        head = lam[0:8] + jnp.where(first_lane, extra, 0.0)
        return jnp.concatenate([head, lam[8:]], axis=0).astype(jnp.bfloat16)

    def mixed(lam, y):
        pair = inv_pair[y]
        both = jnp.dot(split(lam), jnp.concatenate([pair, pair], axis=0), preferred_element_type=jnp.float32)
        mu = both[:, :levels] + both[:, levels:]
        return mu, diff_ref[y] * mu

    def neighbours_in():
        @pl.when(has_s)
        def _():
            for copy in north_to:
                copy.wait_recv()
            fresh, g = mixed(in_s[1].astype(jnp.float32), 0)
            mu_ref[0] += fresh
            flux(0)[1, EDGE:EDGE + nx, :] += g
            in_w[ny:ny + 1, :] += knots[0, 0:1, :]
            in_w[0:1, :] += knots[0, 2:3, :]
            in_e[0:1, :] += knots[2, 4:5, :] + knots[3, 0:1, :]
            lam = beside(in_s[0].astype(jnp.float32), knots[0, 1:2, :])
            mu = jnp.dot(lam, inv_halo[1], preferred_element_type=jnp.float32)
            flux(0)[0, EDGE:EDGE + nx, :] = diff_rows[1].astype(jnp.float32) * mu

        @pl.when(has_n)
        def _():
            for copy in south_to:
                copy.wait_recv()
            lam = beside(in_n[...].astype(jnp.float32) + edge_n[1].astype(jnp.float32),
                         knots[1, 3:4, :] + in_w[2 * ny:2 * ny + 1, :])
            mu = jnp.dot(lam, inv_halo[0], preferred_element_type=jnp.float32)
            flux(0)[ny + 1, EDGE:EDGE + nx, :] = diff_rows[0].astype(jnp.float32) * mu

    def row(n, y):
        if n > 0:
            return mixed(stencil(flux(n - 1), y), y)
        rows = pl.ds(pl.multiple_of(y * pitch, 8), nx)
        return mixed((acc0[rows, :] + acc1[rows, :]) + (acc2[rows, :] + acc3[rows, :]), y)

    def columns_in(n, c):
        for side in range(2):
            cols(n, side, c).wait_recv()
        for r in range(CHUNK):
            y = c * CHUNK + r
            flux(n)[y + 1, EDGE - 1:EDGE, :] = col_recv[n, 0, pl.ds(y, 1), :]
            flux(n)[y + 1, EDGE + nx:EDGE + nx + 1, :] = col_recv[n, 1, pl.ds(y, 1), :]

    def rows_in(n):
        @pl.when(has_s)
        def _():
            rowcopy(n, 0).wait_recv()
            flux(n)[0, EDGE:EDGE + nx, :] = row_recv[n, 0].astype(jnp.float32)

        @pl.when(has_n)
        def _():
            rowcopy(n, 1).wait_recv()
            flux(n)[ny + 1, EDGE:EDGE + nx, :] = row_recv[n, 1].astype(jnp.float32)

    def north_out(n):
        @pl.when(has_n)
        def _():
            rowcopy(n, 0).start()

    def south_out(n):
        @pl.when(has_s)
        def _():
            rowcopy(n, 1).start()

    for n in range(STEPS):
        if n > 0:
            if n > 1:
                columns_in(n - 1, chunks - 1)
                columns_in(n - 1, 0)
                rows_in(n - 1)
            row_send[n, 0] = row(n, ny - 1)[1].astype(row_send.dtype)
            row_send[n, 1] = row(n, 0)[1].astype(row_send.dtype)
            north_out(n)
            south_out(n)

        @pl.loop(0, chunks)
        def _(i):
            c = lax.rem(i + chunks - 1, chunks)
            if n > 1:

                @pl.when(i > 1)
                def _():
                    columns_in(n - 1, c)

            for r in range(CHUNK):
                y = c * CHUNK + r
                mu, g = row(n, y)
                mu_ref[y] = mu
                flux(n)[y + 1, pl.ds(EDGE, nx), :] = g
                if n > 0:
                    col_send[n, 0, pl.ds(y, 1), :] = g[nx - 1:nx]
                    col_send[n, 1, pl.ds(y, 1), :] = g[0:1]

            if n > 0:
                for side in range(2):
                    cols(n, side, c).start()

        if n == 0:
            for copy in across:
                copy.wait_recv()

            @pl.loop(0, chunks)
            def _(i):
                c = chunks - 1 - i
                pl.when(i == chunks - 1)(neighbours_in)
                for r in range(CHUNK):
                    sides(c * CHUNK + r)

    last = STEPS - 1

    out_pitch = out_ref.shape[0] // nx
    nothing = jnp.zeros((1, levels), jnp.float32)
    g_last[0] = zeros
    g_last[ny + 1] = zeros

    @pl.loop(0, chunks)
    def _(c):
        for r in range(CHUNK):
            y = c * CHUNK + r
            g_last[y + 1, EDGE - 1:EDGE, :] = nothing
            g_last[y + 1, EDGE + nx:EDGE + nx + 1, :] = nothing

    @pl.loop(0, chunks)
    def _(c):
        for r in range(CHUNK):
            y = c * CHUNK + r
            out_ref[pl.ds(y, nx, stride=out_pitch), :] = stencil(g_last, y)

    @pl.loop(0, chunks)
    def _(c):
        for side in range(2):
            cols(last, side, c).wait_recv()

    east_edge = (nx - 1) * out_pitch
    out_ref[0:ny, :] += col_recv[last, 0]
    out_ref[east_edge:east_edge + ny, :] += col_recv[last, 1]

    @pl.when(has_s)
    def _():
        rowcopy(last, 0).wait_recv()
        out_ref[pl.ds(0, nx, stride=out_pitch), :] += row_recv[last, 0].astype(jnp.float32)

    @pl.when(has_n)
    def _():
        rowcopy(last, 1).wait_recv()
        out_ref[pl.ds(ny - 1, nx, stride=out_pitch), :] += row_recv[last, 1].astype(jnp.float32)

    @pl.when(has_s)
    def _():
        for n in range(1, STEPS):
            rowcopy(n, 1).wait_send()
        for copy in south_to:
            copy.wait_send()

    @pl.when(has_n)
    def _():
        for n in range(1, STEPS):
            rowcopy(n, 0).wait_send()
        for copy in north_to:
            copy.wait_send()

    for copy in across:
        copy.wait_send()
    for n in range(1, STEPS):

        @pl.loop(0, chunks)
        def _(c):
            for side in range(2):
                cols(n, side, c).wait_send()


def steps(accs, edges, diffusion, inverse, halos, n_gx, n_gy, space=None):
    ny, nx, levels = diffusion.shape
    vm = pltpu.VMEM
    chunks = ny // CHUNK
    dma = pltpu.SemaphoreType.DMA
    make = space or (lambda s, d: jax.ShapeDtypeStruct(s, d))
    return pl.pallas_call(
        functools.partial(steps_body, n_gx, n_gy),
        out_shape=make((nx * (ny + 8), levels), jnp.float32),
        in_specs=[pl.BlockSpec(memory_space=vm)] * (10 + ACCS),
        out_specs=pl.BlockSpec(memory_space=vm),
        scratch_shapes=[
            vm((ny, nx, levels), jnp.float32),
            vm((ny + 2, nx + 2 * EDGE, levels), jnp.float32),
            vm((ny + 2, nx + 2 * EDGE, levels), jnp.float32),
            vm((STEPS, 2, ny, levels), jnp.float32),
            vm((STEPS, 2, ny, levels), jnp.float32),
            vm((STEPS, 2, nx, levels), jnp.bfloat16),
            vm((STEPS, 2, nx, levels), jnp.bfloat16),
            vm((2 * ny + 8, levels), jnp.float32),
            vm((ny, levels), jnp.float32),
            vm((2, nx, levels), jnp.bfloat16),
            vm((nx, levels), jnp.bfloat16),
            vm((4, 8, levels), jnp.float32),
            dma((8,)), dma((8,)),
            dma((STEPS, 2, chunks)), dma((STEPS, 2, chunks)), dma((STEPS, 2)), dma((STEPS, 2)),
        ],
        compiler_params=pltpu.CompilerParams(
            collective_id=1, has_side_effects=True, vmem_limit_bytes=17 * 1024 * 1024),
        name="steps",
    )(*accs, *edges, diffusion, inverse, *halos)


def finish_body(parts, stage, out_ref, sems):
    nx, ny, levels = out_ref.shape
    wide = stage.reshape(nx, stage.shape[0] // nx, levels)
    step = nx // parts
    copies = [
        pltpu.make_async_copy(wide.at[k * step:(k + 1) * step, 0:ny, :], out_ref.at[k * step:(k + 1) * step], sems.at[k])
        for k in range(parts)
    ]
    for copy in copies:
        copy.start()
    for copy in copies:
        copy.wait()


def finish(stage, nx, ny):
    levels = stage.shape[1]
    parts = 8
    return pl.pallas_call(
        functools.partial(finish_body, parts),
        out_shape=jax.ShapeDtypeStruct((nx, ny, levels), jnp.float32),
        in_specs=[pl.BlockSpec(memory_space=pltpu.VMEM)],
        out_specs=pl.BlockSpec(memory_space=pltpu.HBM),
        scratch_shapes=[pltpu.SemaphoreType.DMA((parts,))],
        compiler_params=pltpu.CompilerParams(vmem_limit_bytes=1024 * 1024),
        name="finish",
    )(stage)


def shards(n_gx, n_gy, state, diffusion, vert_inverse, profiles, counts, cell_lon, cell_lat, weight_slot):
    nx, ny, _ = state.shape
    got, got_meta, diffusion, inverse, *rest = exchange(
        counts, profiles, cell_lon, cell_lat, weight_slot, state, diffusion, vert_inverse, ny + 1, n_gx, n_gy)
    made = scatter(got, got_meta, rest[3:], nx, ny)
    stage = steps(made[:ACCS], made[ACCS:], diffusion, inverse, rest[:3], n_gx, n_gy, pltpu.VMEM)
    return finish(stage, nx, ny)


def solution(mesh):
    return jax.shard_map(
        functools.partial(shards, mesh.shape["gx"], mesh.shape["gy"]),
        mesh=mesh,
        in_specs=(
            P("gx", "gy", None),
            P("gx", "gy", None),
            P("gy", None, None),
            P(("gx", "gy"), None),
            P(("gx", "gy"), None),
            P(("gx", "gy")),
            P(("gx", "gy")),
            P(None, ("gx", "gy")),
        ),
        out_specs=P("gx", "gy", None),
        check_vma=False,
    )
```

```python
import functools

import jax
import jax.numpy as jnp
from jax import lax
from jax.experimental import pallas as pl
from jax.experimental.pallas import tpu as pltpu
from jax.sharding import PartitionSpec as P

CAP = 16
MESH = pl.DeviceIdType.MESH

ACCS = 4
EDGE = 8
CLEAR = 64


def split(value):
    high = value.astype(jnp.bfloat16)
    low = (value - high.astype(jnp.float32)).astype(jnp.bfloat16)
    return jnp.concatenate([high, low], axis=1)


def exchange_body(n_gx, n_gy, unused_lat, counts_ref, prof_ref, lon_ref, lat_ref, weight_ref, state_ref, diff_ref,
                  inv_ref, prof_out, meta_out, diff_out, inv_out, inv_halo, diff_rows, diff_cols, acc0, acc1, acc2, acc3,
                  counts, prof, lon, lat, weight, wide, table, prof_send, meta_send, inv_stage, state_stage, diff_stage, row_stage, high_stage,
                  load_sem, psend, precv, msend, mrecv, hsend, hrecv):
    held, levels = prof_ref.shape
    peers = prof_out.shape[0]
    nx, ny, _ = state_ref.shape
    pitch = state_stage.shape[0] // nx
    wide_x = nx + EDGE
    gx = lax.axis_index("gx")
    gy = lax.axis_index("gy")
    me = gx * n_gy + gy
    small = [
        pltpu.make_async_copy(src, dst, load_sem.at[k])
        for k, (src, dst) in enumerate(
            [(counts_ref, counts), (prof_ref, prof), (lon_ref, lon), (lat_ref, lat), (weight_ref, weight)])
    ]
    large = [
        pltpu.make_async_copy(diff_ref, diff_stage.reshape(nx, pitch, levels).at[:, 0:ny, :], load_sem.at[5]),
        pltpu.make_async_copy(inv_ref, inv_stage, load_sem.at[6]),
        pltpu.make_async_copy(state_ref, state_stage.reshape(nx, pitch, levels).at[:, 0:ny, :], load_sem.at[7]),
    ]
    for copy in small:
        copy.start()

    turn = (2, 1, 3, 0)
    depth = n_gy // 4
    near = [lax.rem(lax.rem(gy, 4) + dy, 4) for dy in range(4)]
    far = [lax.rem(lax.div(gy, 4) + dz, depth) * 4 for dz in range(depth)]
    lines = [far[dz] + near[dy] for dz in turn[:depth] for dy in turn if (dz, dy) != (0, 0)]

    def each_peer(do):
        @pl.loop(0, n_gx)
        def _(k):
            x = lax.rem(gx + n_gx // 2 + k, n_gx)
            for y in lines:
                do(x, y)

        for dx in range(1, n_gx):
            do(lax.rem(gx + dx, n_gx), gy)

    barrier = pltpu.get_barrier_semaphore()
    each_peer(lambda x, y: pl.semaphore_signal(barrier, inc=1, device_id=(x, y), device_id_type=MESH))

    for copy in small:
        copy.wait()
    for copy in large:
        copy.start()
    blocks = held // 128
    wide[0:held, :] = prof[...].astype(jnp.float32)
    wide[held:held + CAP, :] = jnp.zeros((CAP, levels), jnp.float32)
    for b in range(blocks):
        table[b, 0:1, :] = lon[b:b + 1, :]
        table[b, 1:2, :] = lat[b:b + 1, :]
        table[b, 2:4, :] = weight[:, b * 128:(b + 1) * 128]
        table[b, 4:8, :] = jnp.zeros((4, 128), jnp.int32)
    for b in range(blocks, blocks + 2):
        table[b] = jnp.zeros((8, 128), jnp.int32)
    lane = lax.broadcasted_iota(jnp.int32, (8, 128), 1)
    field = lax.broadcasted_iota(jnp.int32, (8, 128), 0)

    def one(d, start):
        count = counts[0, d]
        prof_send[d] = wide[pl.ds(start, CAP), :].astype(jnp.bfloat16)
        at = lax.rem(start, 128)
        b = lax.div(start, 128)
        back = lax.rem(128 - at, 128)
        here = pltpu.roll(table[b], back, 1)
        there = pltpu.roll(table[b + 1], back, 1)
        got = jnp.where(lane < 128 - at, here, there)
        got = jnp.where((field == 1) & (lane >= count), unused_lat, got)
        row = jnp.where((field == 0) & (lane < CAP), got, 0)
        for f in range(1, 4):
            moved = pltpu.roll(got, f * CAP, 1)
            row = row + jnp.where((field == f) & (lane >= f * CAP) & (lane < (f + 1) * CAP), moved, 0)
        meta_send[pl.ds(d, 1), :] = jnp.sum(row, axis=0, keepdims=True)
        return start + count

    lax.fori_loop(0, peers, one, jnp.int32(0), unroll=16)

    def remote(src, dst, ssem, rsem, x, y):
        return pltpu.make_async_remote_copy(
            src_ref=src, dst_ref=dst, send_sem=ssem, recv_sem=rsem, device_id=(x, y), device_id_type=MESH)

    has_n = gy < n_gy - 1
    has_s = gy > 0
    up = jnp.minimum(gy + 1, n_gy - 1)
    down = jnp.maximum(gy - 1, 0)
    e = lax.rem(gx + 1, n_gx)
    w = lax.rem(gx + n_gx - 1, n_gx)

    def halo(k, src, dst, x, y):
        return remote(src, dst, hsend.at[k], hrecv.at[k], x, y)

    to_e = halo(0, diff_stage.at[(nx - 1) * pitch:(nx - 1) * pitch + ny], diff_cols.at[0], e, gy)
    to_w = halo(1, diff_stage.at[0:ny], diff_cols.at[1], w, gy)
    to_n = [halo(2, row_stage.at[1], diff_rows.at[1], gx, up),
            halo(3, high_stage.at[1], inv_halo.at[1], gx, up)]
    to_s = [halo(4, row_stage.at[0], diff_rows.at[0], gx, down),
            halo(5, high_stage.at[0], inv_halo.at[0], gx, down)]
    pl.semaphore_wait(barrier, peers - 1)

    def send(x, y):
        to = x * n_gy + y
        remote(prof_send.at[to], prof_out.at[me], psend, precv, x, y).start()
        remote(meta_send.at[pl.ds(to, 1)], meta_out.at[pl.ds(me, 1)], msend, mrecv, x, y).start()

    each_peer(send)
    large[0].wait()
    large[1].wait()
    for k, y in ((0, 0), (1, ny - 1)):
        row_stage[k] = diff_stage[pl.ds(y, nx, stride=pitch), :].astype(jnp.bfloat16)
        high_stage[k] = inv_stage[y].astype(jnp.bfloat16)
    to_e.start()
    to_w.start()

    @pl.when(has_n)
    def _():
        for copy in to_n:
            copy.start()

    @pl.when(has_s)
    def _():
        for copy in to_s:
            copy.start()

    prof_out[me] = prof_send[me]
    meta_out[pl.ds(me, 1), :] = meta_send[pl.ds(me, 1), :]
    empty = jnp.zeros((CLEAR, levels), jnp.float32)

    @pl.loop(0, acc1.shape[0] // CLEAR)
    def _(i):
        rows = pl.ds(pl.multiple_of(i * CLEAR, CLEAR), CLEAR)
        for acc in (acc1, acc2, acc3):
            acc[rows, :] = empty

    @pl.loop(0, ny, unroll=4)
    def _(y):
        inv_out[y] = split(inv_stage[y])

    large[2].wait()
    margin = jnp.zeros((EDGE, levels), jnp.float32)

    @pl.loop(0, ny, unroll=2)
    def _(y):
        first = pl.multiple_of(y * wide_x, 8)
        acc0[pl.ds(first, nx), :] = state_stage[pl.ds(y, nx, stride=pitch), :]
        acc0[pl.ds(first + nx, EDGE), :] = margin
        diff_out[y] = diff_stage[pl.ds(y, nx, stride=pitch), :]

    tail = acc0.shape[0] - ny * wide_x
    acc0[ny * wide_x:, :] = jnp.zeros((tail, levels), jnp.float32)
    n = peers - 1
    whole_p = remote(prof_send.at[0:n], prof_out.at[0:n], psend, precv, gx, gy)
    whole_m = remote(meta_send.at[0:n], meta_out.at[0:n], msend, mrecv, gx, gy)
    whole_p.wait_recv()
    whole_m.wait_recv()
    whole_p.wait_send()
    whole_m.wait_send()
    for copy in (to_e, to_w):
        copy.wait_send()
        copy.wait_recv()

    @pl.when(has_n)
    def _():
        for copy in to_n:
            copy.wait_send()
        for copy in to_s:
            copy.wait_recv()

    @pl.when(has_s)
    def _():
        for copy in to_s:
            copy.wait_send()
        for copy in to_n:
            copy.wait_recv()


def exchange(counts, prof, lon, lat, weight, state, diff, inv, unused_lat, n_gx, n_gy):
    held, levels = prof.shape
    nx, ny, _ = state.shape
    peers = counts.shape[1]
    vm = pltpu.VMEM
    dma = pltpu.SemaphoreType.DMA
    hbm = functools.partial(pltpu.with_memory_space_constraint, memory_space=pltpu.HBM)
    args = (counts, prof, lon.reshape(-1, 128), lat.reshape(-1, 128), weight, state, diff, inv)
    pitched = (nx * (ny + 8), levels)
    rows = -(-(ny + 3) * (nx + EDGE) // CLEAR) * CLEAR
    return pl.pallas_call(
        functools.partial(exchange_body, n_gx, n_gy, unused_lat),
        out_shape=(
            vm((peers, CAP, levels), jnp.bfloat16),
            vm((peers, 128), jnp.int32),
            vm((ny, nx, levels), jnp.float32),
            vm((ny, levels, 2 * levels), jnp.bfloat16),
            vm((2, levels, levels), jnp.bfloat16),
            vm((2, nx, levels), jnp.bfloat16),
            vm((2, ny, levels), jnp.float32),
            *[vm((rows, levels), jnp.float32)] * ACCS,
        ),
        in_specs=[pl.BlockSpec(memory_space=pltpu.HBM)] * 8,
        out_specs=[pl.BlockSpec(memory_space=vm)] * (7 + ACCS),
        scratch_shapes=[
            pltpu.SMEM((1, peers), jnp.int32),
            vm((held, levels), jnp.bfloat16),
            vm((held // 128, 128), jnp.int32),
            vm((held // 128, 128), jnp.int32),
            vm((2, held), jnp.int32),
            vm((held + CAP, levels), jnp.float32),
            vm((held // 128 + 2, 8, 128), jnp.int32),
            vm((peers, CAP, levels), jnp.bfloat16),
            vm((peers, 128), jnp.int32),
            vm((ny, levels, levels), jnp.float32),
            vm(pitched, jnp.float32),
            vm(pitched, jnp.float32),
            vm((2, nx, levels), jnp.bfloat16),
            vm((2, levels, levels), jnp.bfloat16),
            dma((8,)), dma, dma, dma, dma, dma((6,)), dma((6,)),
        ],
        compiler_params=pltpu.CompilerParams(
            collective_id=0, has_side_effects=True, vmem_limit_bytes=17 * 1024 * 1024),
        name="exchange",
    )(*[hbm(a) for a in args])


SLOTS = 64


def scatter_body(nx, ny, prof_ref, meta_ref, *rest):
    peers, cap, levels = prof_ref.shape
    pitch = nx + EDGE
    accs = rest[ACCS:2 * ACCS]
    edge_e, edge_w, edge_n, edge_s, knot, table, index_v, index_s, index_sem = rest[2 * ACCS:]
    meta = meta_ref[...]
    lat_up = pltpu.roll(meta, 128 - cap, 1)
    index_v[...] = lat_up * pitch + meta
    index_copy = pltpu.make_async_copy(index_v, index_s, index_sem)
    index_copy.start()
    group = 8
    lane = lax.broadcasted_iota(jnp.int32, (group, cap, 128), 2)
    slot = lax.broadcasted_iota(jnp.int32, (group, cap, 128), 1)
    own = (lane % cap == slot).astype(jnp.float32)
    r = lax.broadcasted_iota(jnp.int32, (128, 2 * levels), 0) // cap
    c = lax.broadcasted_iota(jnp.int32, (128, 2 * levels), 1) // levels
    pick = (r == c + 2).astype(jnp.bfloat16)

    @pl.loop(0, peers // group, unroll=4)
    def _(i):
        m = meta_ref[pl.ds(pl.multiple_of(i * group, group), group), :].astype(jnp.float32)
        spread = (m[:, None, :] * own).reshape(group * cap, 128).astype(jnp.bfloat16)
        frac = jnp.dot(spread, pick, preferred_element_type=jnp.float32) * (1.0 / SLOTS)
        fx = frac[:, :levels]
        fy = frac[:, levels:]
        p = prof_ref[pl.ds(i * group, group)].reshape(group * cap, levels).astype(jnp.float32)
        p1 = p * fx
        p0 = p - p1
        q01 = p0 * fy
        q11 = p1 * fy
        base = i * (group * cap * 4)
        n = group * cap
        table[pl.ds(base, n, stride=4), :] = p0 - q01
        table[pl.ds(base + 1, n, stride=4), :] = p1 - q11
        table[pl.ds(base + 2, n, stride=4), :] = q01
        table[pl.ds(base + 3, n, stride=4), :] = q11

    index_copy.wait()

    @pl.loop(0, peers)
    def _(s):
        first = pl.multiple_of(s * (cap * 4), cap * 4)
        for k in range(0, cap, ACCS):
            for j in range(ACCS):
                at = index_s[s, k + j]
                row = first + (k + j) * 4
                acc = accs[j]
                acc[pl.ds(at, 2), :] += table[pl.ds(row, 2), :]
                acc[pl.ds(at + pitch, 2), :] += table[pl.ds(row + 2, 2), :]

    def total(at, n):
        out = accs[0][pl.ds(at, n), :]
        for acc in accs[1:]:
            out = out + acc[pl.ds(at, n), :]
        return out

    @pl.loop(0, ny, unroll=8)
    def _(y):
        first = pl.multiple_of(y * pitch, 8)
        edge_w[pl.ds(y, 1), :] = total(first, 8)[0:1]
        edge_e[pl.ds(y, 1), :] = total(first + nx - 8, 8)[7:8]
        edge_e[pl.ds(ny + y, 1), :] = total(first + nx, 8)[0:1]

    edge_s[...] = total(0, nx).astype(edge_s.dtype)
    edge_n[0] = total((ny - 1) * pitch, nx).astype(edge_n.dtype)
    edge_n[1] = total(ny * pitch, nx).astype(edge_n.dtype)
    corner = total(ny * pitch + nx, 8)
    edge_e[2 * ny:2 * ny + 8, :] = corner
    knot[0:1, :] = corner[0:1]
    knot[1:2, :] = total((ny - 1) * pitch + nx, 8)[0:1]
    knot[2:3, :] = total(ny * pitch + nx - 8, 8)[7:8]
    knot[3:4, :] = total(nx, 8)[0:1]
    knot[4:5, :] = total(ny * pitch, 8)[0:1]
    knot[5:8, :] = jnp.zeros((3, levels), jnp.float32)


def scatter(prof, meta, accs, nx, ny):
    peers, cap, levels = prof.shape
    vm = pltpu.VMEM
    block = pl.BlockSpec(memory_space=vm)
    return pl.pallas_call(
        functools.partial(scatter_body, nx, ny),
        out_shape=(
            *[vm(accs[0].shape, jnp.float32)] * ACCS,
            vm((2 * ny + 8, levels), jnp.float32),
            vm((ny, levels), jnp.float32),
            vm((2, nx, levels), jnp.bfloat16),
            vm((nx, levels), jnp.bfloat16),
            vm((8, levels), jnp.float32),
        ),
        in_specs=[block] * (2 + ACCS),
        out_specs=[block] * (5 + ACCS),
        scratch_shapes=[
            vm((peers * cap * 4 + 8, levels), jnp.float32),
            vm((peers, 128), jnp.int32),
            pltpu.SMEM((peers, 128), jnp.int32),
            pltpu.SemaphoreType.DMA,
        ],
        input_output_aliases={2 + k: k for k in range(ACCS)},
        compiler_params=pltpu.CompilerParams(vmem_limit_bytes=5 * 1024 * 1024),
        name="scatter",
    )(prof, meta, *accs)


STEPS = 4
CHUNK = 8


def steps_body(n_gx, n_gy, acc0, acc1, acc2, acc3, edge_e, edge_w, edge_n, edge_s, knot,
               diff_ref, inv_pair, inv_halo, diff_rows, diff_cols, out_ref,
               mu_ref, g_last, g_other, col_send, col_recv, row_send, row_recv, in_w, in_e, in_s, in_n, knots,
               spill_send, spill_recv, col_ssem, col_rsem, row_ssem, row_rsem):
    ny, nx, levels = diff_ref.shape
    pitch = nx + EDGE
    gx = lax.axis_index("gx")
    gy = lax.axis_index("gy")
    e = lax.rem(gx + 1, n_gx)
    w = lax.rem(gx + n_gx - 1, n_gx)
    has_n = gy < n_gy - 1
    has_s = gy > 0
    up = jnp.minimum(gy + 1, n_gy - 1)
    down = jnp.maximum(gy - 1, 0)
    barrier = pltpu.get_barrier_semaphore()

    def greet(x, y):
        pl.semaphore_signal(barrier, inc=1, device_id=(x, y), device_id_type=MESH)

    greet(e, gy)
    greet(w, gy)

    @pl.when(has_n)
    def _():
        greet(gx, up)
        greet(e, up)
        greet(w, up)

    @pl.when(has_s)
    def _():
        greet(gx, down)
        greet(e, down)
        greet(w, down)

    pl.semaphore_wait(barrier, 2 + 3 * has_n.astype(jnp.int32) + 3 * has_s.astype(jnp.int32))

    def remote(src, dst, ssem, rsem, x, y):
        return pltpu.make_async_remote_copy(
            src_ref=src, dst_ref=dst, send_sem=ssem, recv_sem=rsem, device_id=(x, y), device_id_type=MESH)

    def spill(k, src, dst, x, y):
        return remote(src, dst, spill_send.at[k], spill_recv.at[k], x, y)

    across = [spill(0, edge_e, in_w, e, gy), spill(1, edge_w, in_e, w, gy)]
    north_to = [spill(2, edge_n, in_s, gx, up), spill(4, knot, knots.at[0], e, up),
                spill(6, knot, knots.at[2], w, up), spill(7, knot, knots.at[3], gx, up)]
    south_to = [spill(3, edge_s, in_n, gx, down), spill(5, knot, knots.at[1], e, down)]
    for copy in across:
        copy.start()

    @pl.when(has_n)
    def _():
        for copy in north_to:
            copy.start()

    @pl.when(has_s)
    def _():
        for copy in south_to:
            copy.start()

    zeros = jnp.zeros((nx + 2 * EDGE, levels), jnp.float32)

    @pl.when(jnp.logical_not(has_s))
    def _():
        g_other[0] = zeros
        g_last[0] = zeros

    @pl.when(jnp.logical_not(has_n))
    def _():
        g_other[ny + 1] = zeros
        g_last[ny + 1] = zeros

    chunks = ny // CHUNK

    def cols(n, side, c):
        rows = pl.ds(pl.multiple_of(c * CHUNK, CHUNK), CHUNK)
        return remote(col_send.at[n, side, rows], col_recv.at[n, side, rows],
                      col_ssem.at[n, side, c], col_rsem.at[n, side, c], e if side == 0 else w, gy)

    def flux(n):
        return g_last if (STEPS - 1 - n) % 2 == 0 else g_other

    def rowcopy(n, side):
        return remote(row_send.at[n, side], row_recv.at[n, side],
                      row_ssem.at[n, side], row_rsem.at[n, side], gx, up if side == 0 else down)

    def stencil(g, y):
        mid = g[y + 1, pl.ds(EDGE, nx), :]
        near = (g[y + 1, pl.ds(EDGE - 1, nx), :] + g[y + 1, pl.ds(EDGE + 1, nx), :]) + (
            g[y, pl.ds(EDGE, nx), :] + g[y + 2, pl.ds(EDGE, nx), :])
        return mu_ref[y] + (near - 4.0 * mid)

    first_lane = lax.broadcasted_iota(jnp.int32, (8, levels), 0) == 0

    side_lane = lax.broadcasted_iota(jnp.int32, (16, levels), 0)

    def sides(y):
        spilled = in_w[pl.ds(ny + y, 1), :]
        west = in_w[pl.ds(y, 1), :]
        east = in_e[pl.ds(y, 1), :] + edge_e[pl.ds(ny + y, 1), :]
        lam = jnp.where(side_lane == 0, spilled, jnp.where(side_lane == 1, west, jnp.where(side_lane == 2, east, 0.0)))
        mu = jnp.dot(lam.astype(jnp.bfloat16), inv_pair[y, :, 0:levels], preferred_element_type=jnp.float32)
        g = flux(0)
        mu_ref[y, 0:1, :] += mu[0:1]
        g[y + 1, EDGE:EDGE + 1, :] += diff_ref[y, 0:1, :] * mu[0:1]
        g[y + 1, EDGE - 1:EDGE, :] = diff_cols[0, pl.ds(y, 1), :] * mu[1:2]
        g[y + 1, EDGE + nx:EDGE + nx + 1, :] = diff_cols[1, pl.ds(y, 1), :] * mu[2:3]

    def beside(lam, extra):
        head = lam[0:8] + jnp.where(first_lane, extra, 0.0)
        return jnp.concatenate([head, lam[8:]], axis=0).astype(jnp.bfloat16)

    def mixed(lam, y):
        pair = inv_pair[y]
        both = jnp.dot(split(lam), jnp.concatenate([pair, pair], axis=0), preferred_element_type=jnp.float32)
        mu = both[:, :levels] + both[:, levels:]
        return mu, diff_ref[y] * mu

    def neighbours_in():
        @pl.when(has_s)
        def _():
            for copy in north_to:
                copy.wait_recv()
            fresh, g = mixed(in_s[1].astype(jnp.float32), 0)
            mu_ref[0] += fresh
            flux(0)[1, EDGE:EDGE + nx, :] += g
            in_w[ny:ny + 1, :] += knots[0, 0:1, :]
            in_w[0:1, :] += knots[0, 2:3, :]
            in_e[0:1, :] += knots[2, 4:5, :] + knots[3, 0:1, :]
            lam = beside(in_s[0].astype(jnp.float32), knots[0, 1:2, :])
            mu = jnp.dot(lam, inv_halo[1], preferred_element_type=jnp.float32)
            flux(0)[0, EDGE:EDGE + nx, :] = diff_rows[1].astype(jnp.float32) * mu

        @pl.when(has_n)
        def _():
            for copy in south_to:
                copy.wait_recv()
            lam = beside(in_n[...].astype(jnp.float32) + edge_n[1].astype(jnp.float32),
                         knots[1, 3:4, :] + in_w[2 * ny:2 * ny + 1, :])
            mu = jnp.dot(lam, inv_halo[0], preferred_element_type=jnp.float32)
            flux(0)[ny + 1, EDGE:EDGE + nx, :] = diff_rows[0].astype(jnp.float32) * mu

    def row(n, y):
        if n > 0:
            return mixed(stencil(flux(n - 1), y), y)
        rows = pl.ds(pl.multiple_of(y * pitch, 8), nx)
        return mixed((acc0[rows, :] + acc1[rows, :]) + (acc2[rows, :] + acc3[rows, :]), y)

    def columns_in(n, c):
        for side in range(2):
            cols(n, side, c).wait_recv()
        for r in range(CHUNK):
            y = c * CHUNK + r
            flux(n)[y + 1, EDGE - 1:EDGE, :] = col_recv[n, 0, pl.ds(y, 1), :]
            flux(n)[y + 1, EDGE + nx:EDGE + nx + 1, :] = col_recv[n, 1, pl.ds(y, 1), :]

    def rows_in(n):
        @pl.when(has_s)
        def _():
            rowcopy(n, 0).wait_recv()
            flux(n)[0, EDGE:EDGE + nx, :] = row_recv[n, 0].astype(jnp.float32)

        @pl.when(has_n)
        def _():
            rowcopy(n, 1).wait_recv()
            flux(n)[ny + 1, EDGE:EDGE + nx, :] = row_recv[n, 1].astype(jnp.float32)

    def north_out(n):
        @pl.when(has_n)
        def _():
            rowcopy(n, 0).start()

    def south_out(n):
        @pl.when(has_s)
        def _():
            rowcopy(n, 1).start()

    for n in range(STEPS):
        if n > 0:
            if n > 1:
                columns_in(n - 1, chunks - 1)
                columns_in(n - 1, 0)
                rows_in(n - 1)
            row_send[n, 0] = row(n, ny - 1)[1].astype(row_send.dtype)
            row_send[n, 1] = row(n, 0)[1].astype(row_send.dtype)
            north_out(n)
            south_out(n)

        @pl.loop(0, chunks)
        def _(i):
            c = lax.rem(i + chunks - 1, chunks)
            if n > 1:

                @pl.when(i > 1)
                def _():
                    columns_in(n - 1, c)

            for r in range(CHUNK):
                y = c * CHUNK + r
                mu, g = row(n, y)
                mu_ref[y] = mu
                flux(n)[y + 1, pl.ds(EDGE, nx), :] = g
                if n > 0:
                    col_send[n, 0, pl.ds(y, 1), :] = g[nx - 1:nx]
                    col_send[n, 1, pl.ds(y, 1), :] = g[0:1]

            if n > 0:
                for side in range(2):
                    cols(n, side, c).start()

        if n == 0:
            for copy in across:
                copy.wait_recv()

            @pl.loop(0, chunks)
            def _(i):
                c = chunks - 1 - i
                pl.when(i == chunks - 1)(neighbours_in)
                for r in range(CHUNK):
                    sides(c * CHUNK + r)

    last = STEPS - 1

    out_pitch = out_ref.shape[0] // nx
    nothing = jnp.zeros((1, levels), jnp.float32)
    g_last[0] = zeros
    g_last[ny + 1] = zeros

    @pl.loop(0, chunks)
    def _(c):
        for r in range(CHUNK):
            y = c * CHUNK + r
            g_last[y + 1, EDGE - 1:EDGE, :] = nothing
            g_last[y + 1, EDGE + nx:EDGE + nx + 1, :] = nothing

    @pl.loop(0, chunks)
    def _(c):
        for r in range(CHUNK):
            y = c * CHUNK + r
            out_ref[pl.ds(y, nx, stride=out_pitch), :] = stencil(g_last, y)

    @pl.loop(0, chunks)
    def _(c):
        for side in range(2):
            cols(last, side, c).wait_recv()

    east_edge = (nx - 1) * out_pitch
    out_ref[0:ny, :] += col_recv[last, 0]
    out_ref[east_edge:east_edge + ny, :] += col_recv[last, 1]

    @pl.when(has_s)
    def _():
        rowcopy(last, 0).wait_recv()
        out_ref[pl.ds(0, nx, stride=out_pitch), :] += row_recv[last, 0].astype(jnp.float32)

    @pl.when(has_n)
    def _():
        rowcopy(last, 1).wait_recv()
        out_ref[pl.ds(ny - 1, nx, stride=out_pitch), :] += row_recv[last, 1].astype(jnp.float32)

    @pl.when(has_s)
    def _():
        for n in range(1, STEPS):
            rowcopy(n, 1).wait_send()
        for copy in south_to:
            copy.wait_send()

    @pl.when(has_n)
    def _():
        for n in range(1, STEPS):
            rowcopy(n, 0).wait_send()
        for copy in north_to:
            copy.wait_send()

    for copy in across:
        copy.wait_send()
    for n in range(1, STEPS):

        @pl.loop(0, chunks)
        def _(c):
            for side in range(2):
                cols(n, side, c).wait_send()


def steps(accs, edges, diffusion, inverse, halos, n_gx, n_gy, space=None):
    ny, nx, levels = diffusion.shape
    vm = pltpu.VMEM
    chunks = ny // CHUNK
    dma = pltpu.SemaphoreType.DMA
    make = space or (lambda s, d: jax.ShapeDtypeStruct(s, d))
    return pl.pallas_call(
        functools.partial(steps_body, n_gx, n_gy),
        out_shape=make((nx * (ny + 8), levels), jnp.float32),
        in_specs=[pl.BlockSpec(memory_space=vm)] * (10 + ACCS),
        out_specs=pl.BlockSpec(memory_space=vm),
        scratch_shapes=[
            vm((ny, nx, levels), jnp.float32),
            vm((ny + 2, nx + 2 * EDGE, levels), jnp.float32),
            vm((ny + 2, nx + 2 * EDGE, levels), jnp.float32),
            vm((STEPS, 2, ny, levels), jnp.float32),
            vm((STEPS, 2, ny, levels), jnp.float32),
            vm((STEPS, 2, nx, levels), jnp.bfloat16),
            vm((STEPS, 2, nx, levels), jnp.bfloat16),
            vm((2 * ny + 8, levels), jnp.float32),
            vm((ny, levels), jnp.float32),
            vm((2, nx, levels), jnp.bfloat16),
            vm((nx, levels), jnp.bfloat16),
            vm((4, 8, levels), jnp.float32),
            dma((8,)), dma((8,)),
            dma((STEPS, 2, chunks)), dma((STEPS, 2, chunks)), dma((STEPS, 2)), dma((STEPS, 2)),
        ],
        compiler_params=pltpu.CompilerParams(
            collective_id=1, has_side_effects=True, vmem_limit_bytes=17 * 1024 * 1024),
        name="steps",
    )(*accs, *edges, diffusion, inverse, *halos)


def finish_body(parts, stage, out_ref, sems):
    nx, ny, levels = out_ref.shape
    wide = stage.reshape(nx, stage.shape[0] // nx, levels)
    step = nx // parts
    copies = [
        pltpu.make_async_copy(wide.at[k * step:(k + 1) * step, 0:ny, :], out_ref.at[k * step:(k + 1) * step], sems.at[k])
        for k in range(parts)
    ]
    for copy in copies:
        copy.start()
    for copy in copies:
        copy.wait()


def finish(stage, nx, ny):
    levels = stage.shape[1]
    parts = 8
    return pl.pallas_call(
        functools.partial(finish_body, parts),
        out_shape=jax.ShapeDtypeStruct((nx, ny, levels), jnp.float32),
        in_specs=[pl.BlockSpec(memory_space=pltpu.VMEM)],
        out_specs=pl.BlockSpec(memory_space=pltpu.HBM),
        scratch_shapes=[pltpu.SemaphoreType.DMA((parts,))],
        compiler_params=pltpu.CompilerParams(vmem_limit_bytes=1024 * 1024),
        name="finish",
    )(stage)


def shards(n_gx, n_gy, state, diffusion, vert_inverse, profiles, counts, cell_lon, cell_lat, weight_slot):
    nx, ny, _ = state.shape
    got, got_meta, diffusion, inverse, *rest = exchange(
        counts, profiles, cell_lon, cell_lat, weight_slot, state, diffusion, vert_inverse, ny + 1, n_gx, n_gy)
    made = scatter(got, got_meta, rest[3:], nx, ny)
    stage = steps(made[:ACCS], made[ACCS:], diffusion, inverse, rest[:3], n_gx, n_gy, pltpu.VMEM)
    return finish(stage, nx, ny)


def solution(mesh):
    return jax.shard_map(
        functools.partial(shards, mesh.shape["gx"], mesh.shape["gy"]),
        mesh=mesh,
        in_specs=(
            P("gx", "gy", None),
            P("gx", "gy", None),
            P("gy", None, None),
            P(("gx", "gy"), None),
            P(("gx", "gy"), None),
            P(("gx", "gy")),
            P(("gx", "gy")),
            P(None, ("gx", "gy")),
        ),
        out_specs=P("gx", "gy", None),
        check_vma=False,
    )
```
